128 devices in a mesh: mx: 8 (over x, core), my: 8 (over y, z_lo), mz: 2 (over z_hi).
Axes of the slice: x: 4, y: 4, z: 4 (z_hi: 2, z_lo: 2; z = z_hi * 2 + z_lo), core: 2. Of those that a mesh axis runs over, the one named last changes fastest.
Arguments:
- force: float32 [3, 128, 256, 256], P(None, 'mx', 'my', 'mz'), may hold values from -6 to 6
- velocity_prev: float32 [3, 128, 256, 256], P(None, 'mx', 'my', 'mz'), may hold values from -2 to 2
- viscosity: float32 [128, 256, 256], P('mx', 'my', 'mz'), may hold values from 0.5 to 8
- strain: float32 [128, 256, 256], P('mx', 'my', 'mz'), may hold values from 0 to 2
- yield_flags: int32 [128, 256, 256], P('mx', 'my', 'mz'), may hold values 0 or 1
- counts: int32 [2], replicated, may hold values from 4 to 6, as said below
- heights: float32 [128, 256], P('mx'), may hold values from 0 to 2
- receivers: int32 [128, 256], P('mx'), may hold values from 0 to 7
Outputs:
- velocity: float32 [3, 128, 256, 256], P(None, 'mx', 'my', 'mz')
- strain_out: float32 [128, 256, 256], P('mx', 'my', 'mz')
- topography: float32 [128, 256], P('mx')
The draws below stay inside these ranges and needn't reach their ends.
Inputs may be any that keep to these rules, and one draw needn't show every extreme that they name: `counts`: some Picard iteration takes 6 Krylov iterations and another takes 6 - 2.
All inputs are finite; a program needn't handle non-finite values. No bound on the sum of `yield_flags` on one device may be relied on, other than what follows from the above.
Results may differ from the reference program's by a relative error of at most 0.0003.
Values sent between devices are 32-bit elements; how exact they have to be, the bound alone decides.
A program may use at most 128 MiB of HBM per device.

```python
import math
import jax
import jax.numpy as jnp
from jax import lax

PICARD = 2
KMAX = 6
SWEEPS = 4
NX = 128
NY = 256
NZ = 256


def draw_counts(key, part):
    base = jax.random.randint(jax.random.fold_in(key, 31), (PICARD,), KMAX - 2, KMAX + 1)
    base = base.at[0].set(KMAX).at[1].set(KMAX - 2)
    return jax.random.permutation(jax.random.fold_in(key, 57), base).astype(jnp.int32)


def plant(entries, own_key, low, top_value):
    index_at = [jax.random.randint(jax.random.fold_in(own_key, axis), (), 0, length) for axis, length in enumerate(entries.shape)]
    widest = entries.shape.index(max(entries.shape))
    beside = index_at[:widest] + [(index_at[widest] + 1) % entries.shape[widest]] + index_at[widest + 1:]
    return entries.at[tuple(index_at)].set(low).at[tuple(beside)].set(top_value)


def steps_of(rng, dims, pieces, least, top_value):
    def one(axis_at, parts):
        steps = jax.random.uniform(jax.random.fold_in(jax.random.fold_in(rng, 6), axis_at), (parts,), jnp.float32, least / len(pieces), top_value / len(pieces))
        return jnp.repeat(jnp.exp(steps), dims[axis_at] // parts).reshape((-1,) + (1,) * (len(dims) - axis_at - 1))

    level = one(*pieces[0])
    for cut in pieces[1:]:
        level = level * one(*cut)
    return level


def bell_draw(key, shape, width, limit, split=(), kind=jnp.bfloat16):
    level = steps_of(key, shape, split, -0.22, 0.18) if split else 1.0
    drawn = jax.random.normal(key, shape, jnp.float32) * width * level
    return jnp.minimum(jnp.maximum(drawn, -limit), limit).astype(kind)


def setup_inputs(seed: int = 0) -> dict:
    key_of = jax.random.split(jax.random.key(seed), 9)
    force = bell_draw(key_of[0], (3, NX, NY, NZ), 1.0, 6.0, ((1, 8), (2, 8), (3, 2)), jnp.float32)
    velocity_prev = bell_draw(key_of[1], (3, NX, NY, NZ), 0.3, 2.0, ((1, 8), (2, 8), (3, 2)), jnp.float32)
    viscosity = jnp.clip(jnp.exp(math.log(8.0) - 2.7725887 * jax.random.uniform(key_of[2], (NX, NY, NZ), jnp.float32) ** steps_of(key_of[2], (NX, NY, NZ), ((0, 8), (1, 8), (2, 2)), -0.2, 0.2)), 0.5, 8.0)
    strain = jnp.clip(2.0 * jax.random.uniform(key_of[3], (NX, NY, NZ), jnp.float32) ** steps_of(key_of[3], (NX, NY, NZ), ((0, 8), (1, 8), (2, 2)), -0.2, 0.2), 0.0, 2.0)
    yield_flags = plant((jax.random.randint(key_of[4], (NX, NY, NZ), 0, 2) < 1).astype(jnp.int32), jax.random.fold_in(key_of[4], 1), 0, 1)
    counts = draw_counts(jax.random.fold_in(key_of[8], 71), 0)
    heights = jnp.clip(2.0 * jax.random.uniform(key_of[6], (NX, NY), jnp.float32) ** steps_of(key_of[6], (NX, NY), ((0, 8),), -0.2, 0.2), 0.0, 2.0)
    receivers = plant(jax.random.randint(key_of[7], (NX, NY), 0, 8), jax.random.fold_in(key_of[7], 1), 0, 7).astype(jnp.int32)
    return {"force": force, "velocity_prev": velocity_prev, "viscosity": viscosity, "strain": strain, "yield_flags": yield_flags, "counts": counts, "heights": heights, "receivers": receivers}


drag_coef = 0.05
cohesion_base = 1.0
weakening = 0.6
critical_strain = 1.0
sin_friction = 0.5
cos_friction = 0.8660254
pressure_gradient = 2.0
rate_floor = 0.1
strain_step = 0.5
uplift_gain = 8.0
surface_step = 0.2
erodibility = 0.5
neighbour_steps = ((-1, -1), (-1, 0), (-1, 1), (0, -1), (0, 1), (1, -1), (1, 0), (1, 1))

def neighbour(padded, dimension, offset):
    window = [slice(None), slice(1, -1), slice(1, -1), slice(1, -1)]
    window[dimension + 1] = slice(1 + offset, padded.shape[dimension + 1] - 1 + offset)
    return padded[tuple(window)]

def pad_cells(field):
    return jnp.pad(field, ((0, 0), (1, 1), (1, 1), (1, 1)))

def apply_padded(padded, eta_padded):
    centre = padded[:, 1:-1, 1:-1, 1:-1]
    eta_centre = eta_padded[:, 1:-1, 1:-1, 1:-1]
    summed = drag_coef * centre
    for dimension in range(3):
        for offset in (-1, 1):
            face_eta = 0.5 * (eta_centre + neighbour(eta_padded, dimension, offset))
            summed = summed + face_eta * (centre - neighbour(padded, dimension, offset))
    return summed

def rate_invariant(padded):
    gradients = [0.5 * (neighbour(padded, dimension, 1) - neighbour(padded, dimension, -1)) for dimension in range(3)]
    summed = jnp.zeros_like(gradients[0][0])
    for outer_axis in range(3):
        for inner_axis in range(3):
            tensor = 0.5 * (gradients[inner_axis][outer_axis] + gradients[outer_axis][inner_axis])
            summed = summed + tensor * tensor
    return jnp.sqrt(0.5 * summed)

def yield_strength(strain, yield_flags, pressure):
    weakened = yield_flags.astype(jnp.float32) * jnp.minimum(strain / critical_strain, 1.0)
    return cohesion_base * (1.0 - weakening * weakened) * cos_friction + pressure * sin_friction

def viscosity_of(strain_rate, viscosity, strength):
    return jnp.minimum(viscosity, strength / (2.0 * jnp.maximum(strain_rate, rate_floor)))

def spread_area(drained, receivers):
    summed = jnp.zeros((drained.shape[0] + 2, drained.shape[1] + 2), drained.dtype)
    for direction, (row_step, col_step) in enumerate(neighbour_steps):
        outflow = jnp.where(receivers == direction, drained, 0.0)
        summed = summed + jnp.pad(outflow, ((1 + row_step, 1 - row_step), (1 + col_step, 1 - col_step)))
    return summed

def finish_topography(heights, padded, receivers, drained, uplift):
    row_count, col_count = heights.shape
    receiver_height = jnp.zeros_like(heights)
    spacing = jnp.zeros_like(heights)
    for direction, (row_step, col_step) in enumerate(neighbour_steps):
        chosen = receivers == direction
        shifted = padded[1 + row_step:1 + row_step + row_count, 1 + col_step:1 + col_step + col_count]
        receiver_height = receiver_height + jnp.where(chosen, shifted, 0.0)
        spacing = spacing + jnp.where(chosen, math.sqrt(row_step * row_step + col_step * col_step), 0.0)
    gradient = jnp.maximum(heights - receiver_height, 0.0) / spacing
    return heights + surface_step * (uplift_gain * uplift - erodibility * jnp.sqrt(drained) * gradient)

def krylov_solve(padded_start, start, force, eta_padded, iteration_limit):
    residual = force - apply_padded(padded_start, eta_padded)
    direction = residual
    solution = start
    current = jnp.sum(residual * residual)
    for iteration in range(KMAX):
        active = iteration < iteration_limit
        applied = apply_padded(pad_cells(direction), eta_padded)
        step_size = current / jnp.sum(direction * applied)
        stepped = jnp.where(active, step_size, 0.0)
        solution = solution + stepped * direction
        residual = residual - stepped * applied
        updated = jnp.sum(residual * residual)
        direction = jnp.where(active, residual + updated / current * direction, direction)
        current = jnp.where(active, updated, current)
    return solution

def reference(force, velocity_prev, viscosity, strain, yield_flags, counts, heights, receivers):
    pressure = pressure_gradient * (NZ - 0.5 - jnp.arange(NZ, dtype=jnp.float32)) / NZ
    strength = yield_strength(strain, yield_flags, pressure)
    velocity = velocity_prev
    for picard_index in range(PICARD):
        padded = pad_cells(velocity)
        effective = viscosity_of(rate_invariant(padded), viscosity, strength)
        eta_padded = pad_cells(effective[None])
        velocity = krylov_solve(padded, velocity, force, eta_padded, counts[picard_index])
    padded = pad_cells(velocity)
    plastic = jnp.maximum(rate_invariant(padded) - strength / (2.0 * viscosity), 0.0)
    strain_out = strain + strain_step * plastic
    uplift = lax.optimization_barrier(jnp.sum(velocity[2], axis=-1)) / NZ
    drained = jnp.ones_like(heights)
    for sweep_index in range(SWEEPS):
        spread = spread_area(drained, receivers)
        drained = 1.0 + spread[1:-1, 1:-1]
    topography = finish_topography(heights, jnp.pad(heights, 1), receivers, drained, uplift)
    return (velocity, strain_out, topography)
```

```python
import functools
import math

import jax
import jax.numpy as jnp
from jax import lax
from jax.experimental import pallas as pl
from jax.experimental.pallas import tpu as pltpu
from jax.sharding import PartitionSpec as P

KMAX = 6
SWEEPS = 4
NXL, NYL, NZL = 16, 32, 128
PADY = 8
LO, HI = PADY, PADY + NYL
BUFY = PADY + NYL + PADY
RIM = 8

drag_coef = 0.05
cohesion_base = 1.0
weakening = 0.6
critical_strain = 1.0
sin_friction = 0.5
cos_friction = 0.8660254
pressure_gradient = 2.0
rate_floor = 0.1
strain_step = 0.5
uplift_gain = 8.0
surface_step = 0.2
erodibility = 0.5
neighbour_steps = ((-1, -1), (-1, 0), (-1, 1), (0, -1), (0, 1), (1, -1), (1, 0), (1, 1))

MESH = pl.DeviceIdType.MESH
U_SET, E_SET = 2, 3
f32 = jnp.float32


def step_kernel(
    counts, px, py, pz,
    force, vel, visc, strain, flags, heights, receivers,
    vout, sout, tout,
    ubuf, ebuf, wbuf, ys, yr, zs, zr, strength, coef, r, p, s, z, q, sums1, sums2, surf, base, tiles,
    face_send, face_recv, one_send, one_recv, two_send, two_recv, surf_send, surf_recv, tile_send, tile_recv,
):
    mx, my, mz = lax.axis_index("mx"), lax.axis_index("my"), lax.axis_index("mz")
    group = py * pz
    place = my * pz + mz
    edge = (NZL - 1) * (1 - mz)

    def at_group(k):
        other = lax.rem(place + k, group)
        return {"my": other // pz, "mz": lax.rem(other, pz)}

    def at_row(k):
        return {"mx": lax.rem(mx + k, px)}

    def lanes(rows):
        return lax.broadcasted_iota(jnp.int32, (rows, NZL), 1)

    def blank(buf, parts):
        zero = jnp.zeros((NYL, NZL), f32)
        row = jnp.zeros((1, NZL), f32)

        def clear(i, _):
            for c in range(parts):
                buf[c, i, LO - 1 : LO, :] = row
                buf[c, i, HI : HI + 1, :] = row
            return 0

        lax.fori_loop(0, NXL + 2, clear, 0)
        for c in range(parts):
            buf[c, 0, LO:HI, :] = zero
            buf[c, NXL + 1, LO:HI, :] = zero

    blank(ubuf, 3)
    blank(ebuf, 1)
    blank(wbuf.at[0], 3)
    blank(wbuf.at[1], 3)
    for kind in range(4):
        for side in range(2):
            for c in range(3):
                yr[kind, side, c] = jnp.zeros((NXL, NZL), f32)
    rows, cols = surf.shape[1:]
    surf[0, 0:RIM, :] = jnp.full((RIM, cols), -1.0, f32)
    surf[0, RIM + NXL :, :] = jnp.full((RIM, cols), -1.0, f32)
    surf[1, 0:RIM, :] = jnp.zeros((RIM, cols), f32)
    surf[1, RIM + NXL :, :] = jnp.zeros((RIM, cols), f32)
    surf[0, RIM : RIM + NXL, :] = receivers[...].astype(f32)
    surf[1, RIM : RIM + NXL, :] = heights[...]

    barrier = pltpu.get_barrier_semaphore()
    for k in range(1, px):
        pl.semaphore_signal(barrier, inc=1, device_id=at_row(k), device_id_type=MESH)
    for k in range(1, group):
        pl.semaphore_signal(barrier, inc=1, device_id=at_group(k), device_id_type=MESH)

    def face_copy(kind, d, src, dst, device):
        return pltpu.make_async_remote_copy(
            src_ref=src, dst_ref=dst, send_sem=face_send.at[kind, d], recv_sem=face_recv.at[kind, d],
            device_id=device, device_id_type=MESH,
        )

    def face_copies(buf, kind, n):
        comps = slice(0, n)
        return (
            (mx < px - 1, mx > 0, 0, buf.at[comps, NXL, LO:HI, :], buf.at[comps, 0, LO:HI, :], {"mx": mx + 1}),
            (mx > 0, mx < px - 1, 1, buf.at[comps, 1, LO:HI, :], buf.at[comps, NXL + 1, LO:HI, :], {"mx": mx - 1}),
            (my < py - 1, my > 0, 2, ys.at[kind, 1, comps], yr.at[kind, 0, comps], {"my": my + 1}),
            (my > 0, my < py - 1, 3, ys.at[kind, 0, comps], yr.at[kind, 1, comps], {"my": my - 1}),
        )

    def depth_copy(kind):
        return face_copy(kind, 4, zs.at[kind], zr.at[kind], {"mz": 1 - mz})

    def start_faces(buf, kind, n):
        depth_copy(kind).start()
        for sends, _, d, src, dst, device in face_copies(buf, kind, n):
            @pl.when(sends)
            def _():
                face_copy(kind, d, src, dst, device).start()

    def finish_faces(buf, kind, n):
        for sends, receives, d, src, dst, device in face_copies(buf, kind, n):
            @pl.when(sends)
            def _():
                face_copy(kind, d, src, dst, device).wait_send()

            @pl.when(receives)
            def _():
                face_copy(kind, d, src, dst, device).wait_recv()
        depth_copy(kind).wait()
        for c in range(n):
            low, high = yr[kind, 0, c], yr[kind, 1, c]
            for x in range(NXL):
                buf[c, x + 1, LO - 1 : LO, :] = low[x : x + 1]
                buf[c, x + 1, HI : HI + 1, :] = high[x : x + 1]

    half = NYL // 2
    lane_half = lanes(half)
    lane_full = lanes(NYL)

    def pack(kind, c, x, plane, held):
        ys[kind, 0, c, pl.ds(x, 1), :] = plane[0:1]
        ys[kind, 1, c, pl.ds(x, 1), :] = plane[NYL - 1 :]
        for part in range(2):
            spot = c * NXL + x + 48 * part
            turned = pltpu.roll(plane[part * half : (part + 1) * half], lax.rem(spot - edge + NZL, NZL), 1)
            held = jnp.where(lane_half == spot, turned, held)
        return held

    no_pack = jnp.zeros((half, NZL), f32)

    def depth_pair(v, arrived, c, x):
        parts = []
        for part in range(2):
            spot = c * NXL + x + 48 * part
            parts.append(pltpu.roll(arrived, lax.rem(edge - spot + NZL, NZL), 1))
        rim = jnp.where(lane_full == edge, jnp.concatenate(parts, axis=0), 0.0)
        below = jnp.where(lane_full == 0, rim, pltpu.roll(v, 1, 1))
        above = jnp.where(lane_full == NZL - 1, rim, pltpu.roll(v, NZL - 1, 1))
        return below, above

    def around(buf, arrived, c, x):
        v = buf[c, x + 1, LO:HI, :]
        below, above = depth_pair(v, arrived, c, x)
        return v, (
            (buf[c, x, LO:HI, :], buf[c, x + 2, LO:HI, :]),
            (buf[c, x + 1, LO - 1 : HI - 1, :], buf[c, x + 1, LO + 1 : HI + 1, :]),
            (below, above),
        )

    def applied(buf, arrived, c, x):
        v, pairs = around(buf, arrived, c, x)
        total = coef[6, x] * v
        for d in range(3):
            total = total - coef[2 * d, x] * pairs[d][0] - coef[2 * d + 1, x] * pairs[d][1]
        return v, total

    def rate_at(x, arrived):
        g = []
        for c in range(3):
            _, pairs = around(ubuf, arrived, c, x)
            g.append([0.5 * (pair[1] - pair[0]) for pair in pairs])
        total = g[0][0] * g[0][0] + g[1][1] * g[1][1] + g[2][2] * g[2][2]
        for a, b in ((0, 1), (0, 2), (1, 2)):
            shear = g[a][b] + g[b][a]
            total = total + 0.5 * (shear * shear)
        return jnp.sqrt(0.5 * total)

    def planes(body, carry, unroll=2):
        return lax.fori_loop(0, NXL, body, carry, unroll=unroll)

    def one_copy(slot, k):
        mine = sums1.at[slot, mx]
        return pltpu.make_async_remote_copy(
            src_ref=mine, dst_ref=mine, send_sem=one_send.at[slot, k], recv_sem=one_recv.at[slot, k],
            device_id=at_row(k), device_id_type=MESH,
        )

    def two_copy(slot, k):
        mine = sums2.at[slot, place]
        return pltpu.make_async_remote_copy(
            src_ref=mine, dst_ref=mine, send_sem=two_send.at[slot, k], recv_sem=two_recv.at[slot, k],
            device_id=at_group(k), device_id_type=MESH,
        )

    def start_sums(slot, gg, dd):
        sums1[slot, mx] = jnp.concatenate(
            [jnp.sum(gg, axis=0, keepdims=True), jnp.sum(dd, axis=0, keepdims=True)], axis=0
        )
        for k in range(1, px):
            one_copy(slot, k).start()

    def middle_sums(slot):
        for k in range(1, px):
            one_copy(slot, k).wait()
        sums2[slot, place] = jnp.sum(sums1[slot], axis=0)
        for k in range(1, group):
            two_copy(slot, k).start()

    def finish_sums(slot):
        for k in range(1, group):
            two_copy(slot, k).wait()
        both = jnp.sum(jnp.sum(sums2[slot], axis=0), axis=1, keepdims=True)
        both = jnp.broadcast_to(both, (2, NZL))
        return both[0:1], both[1:2]

    def load(x, held):
        for c in range(3):
            plane = vel[c, x]
            ubuf[c, x + 1, LO:HI, :] = plane
            held = pack(U_SET, c, x, plane, held)
        return held

    zs[U_SET] = planes(load, no_pack)
    pl.semaphore_wait(barrier, px - 1 + group - 1)
    start_faces(ubuf, U_SET, 3)

    def surf_copy(d):
        if d == 0:
            src, dst, device = surf.at[:, NXL : NXL + RIM], surf.at[:, 0:RIM], {"mx": mx + 1}
        else:
            src, dst, device = surf.at[:, RIM : 2 * RIM], surf.at[:, RIM + NXL : RIM + NXL + RIM], {"mx": mx - 1}
        return pltpu.make_async_remote_copy(
            src_ref=src, dst_ref=dst, send_sem=surf_send.at[d], recv_sem=surf_recv.at[d],
            device_id=device, device_id_type=MESH,
        )

    for d, sends in ((0, mx < px - 1), (1, mx > 0)):
        @pl.when(sends)
        def _():
            surf_copy(d).start()

    depth_at = mz * NZL + lane_full
    pressure = pressure_gradient * (pz * NZL - 0.5 - depth_at.astype(f32)) / (pz * NZL)

    def strengthen(x, _):
        weak = flags[x].astype(f32) * jnp.minimum(strain[x] / critical_strain, 1.0)
        strength[x] = cohesion_base * (1.0 - weakening * weak) * cos_friction + pressure * sin_friction
        for c in range(3):
            zero = jnp.zeros((NYL, NZL), f32)
            p[c, x] = zero
            s[c, x] = zero
            z[c, x] = zero
        return 0

    planes(strengthen, 0)

    for d, sends, receives in ((0, mx < px - 1, mx > 0), (1, mx > 0, mx < px - 1)):
        @pl.when(sends)
        def _():
            surf_copy(d).wait_send()

        @pl.when(receives)
        def _():
            surf_copy(d).wait_recv()

    code = surf[0]
    col = lax.broadcasted_iota(jnp.int32, (rows, cols), 1)

    def turned(block, row_step, col_step):
        if col_step:
            block = pltpu.roll(block, col_step % cols, 1)
        if row_step:
            block = pltpu.roll(block, row_step % rows, 0)
        return block

    drained = jnp.ones((rows, cols), f32)
    for _ in range(SWEEPS):
        total = jnp.ones((rows, cols), f32)
        for direction, (row_step, col_step) in enumerate(neighbour_steps):
            chosen = code == float(direction)
            if col_step:
                chosen = chosen & (col != (cols - 1 if col_step > 0 else 0))
            total = total + turned(jnp.where(chosen, drained, 0.0), row_step, col_step)
        drained = total
    height = surf[1]
    below = jnp.zeros((rows, cols), f32)
    spacing = jnp.ones((rows, cols), f32)
    for direction, (row_step, col_step) in enumerate(neighbour_steps):
        chosen = code == float(direction)
        seen = chosen
        if col_step:
            seen = seen & (col != (cols - 1 if col_step > 0 else 0))
        below = below + jnp.where(seen, turned(height, -row_step, -col_step), 0.0)
        if row_step and col_step:
            spacing = jnp.where(chosen, math.sqrt(2.0), spacing)
    slope = jnp.maximum(height - below, 0.0) / spacing
    ground = height - (surface_step * erodibility) * jnp.sqrt(drained) * slope
    base[...] = ground[RIM : RIM + NXL]

    for picard, count in enumerate(counts):
        if picard:
            def resend(x, held):
                for c in range(3):
                    held = pack(U_SET, c, x, ubuf[c, x + 1, LO:HI, :], held)
                return held

            zs[U_SET] = planes(resend, no_pack)
            start_faces(ubuf, U_SET, 3)
        finish_faces(ubuf, U_SET, 3)
        u_rim = zr[U_SET]

        def soften(x, held):
            rate = rate_at(x, u_rim)
            eta = jnp.minimum(visc[x], strength[x] / (2.0 * jnp.maximum(rate, rate_floor)))
            ebuf[0, x + 1, LO:HI, :] = eta
            return pack(E_SET, 0, x, eta, held)

        zs[E_SET] = planes(soften, no_pack)
        start_faces(ebuf, E_SET, 1)
        finish_faces(ebuf, E_SET, 1)
        e_rim = zr[E_SET]

        def begin(x, held):
            eta, pairs = around(ebuf, e_rim, 0, x)
            total = jnp.full((NYL, NZL), drag_coef, f32)
            for d in range(3):
                for side in range(2):
                    face = 0.5 * (eta + pairs[d][side])
                    coef[2 * d + side, x] = face
                    total = total + face
            coef[6, x] = total
            for c in range(3):
                _, au = applied(ubuf, u_rim, c, x)
                plane = force[c, x] - au
                r[c, x] = plane
                wbuf[0, c, x + 1, LO:HI, :] = plane
                held = pack(0, c, x, plane, held)
            return held

        zs[0] = planes(begin, no_pack, 1)
        start_faces(wbuf.at[0], 0, 3)
        finish_faces(wbuf.at[0], 0, 3)
        r_rim = zr[0]
        nothing = jnp.zeros((NYL, NZL), f32)

        def first(x, carry):
            held, gg, dd = carry
            for c in range(3):
                v, w = applied(wbuf.at[0], r_rim, c, x)
                wbuf[1, c, x + 1, LO:HI, :] = w
                gg = gg + v * v
                dd = dd + v * w
                held = pack(1, c, x, w, held)
            return held, gg, dd

        held, gg, dd = planes(first, (no_pack, nothing, nothing))
        zs[1] = held
        start_sums(0, gg, dd)
        start_faces(wbuf.at[1], 1, 3)

        def scalars(i, gamma, delta, gamma_old, alpha_old):
            beta = jnp.where(i == 0, 0.0, gamma / gamma_old)
            alpha = gamma / (delta - beta * gamma / alpha_old)
            return alpha, beta

        def iterate(i, carry):
            gamma_old, alpha_old = carry
            now, later = lax.rem(i + 1, 2), lax.rem(i, 2)
            w_now, w_later = wbuf.at[now], wbuf.at[later]
            slot = lax.rem(i, 2)
            middle_sums(slot)
            finish_faces(w_now, now, 3)
            rim = zr[now]

            def again(x, _):
                for c in range(3):
                    q[c, x] = applied(w_now, rim, c, x)[1]
                return 0

            planes(again, 0)
            gamma, delta = finish_sums(slot)
            alpha, beta = scalars(i, gamma, delta, gamma_old, alpha_old)

            def update(x, carry):
                held, gg, dd = carry
                for c in range(3):
                    w = w_now[c, x + 1, LO:HI, :]
                    z_new = q[c, x] + beta * z[c, x]
                    s_new = w + beta * s[c, x]
                    r_old = r[c, x]
                    p_new = r_old + beta * p[c, x]
                    r_new = r_old - alpha * s_new
                    w_new = w - alpha * z_new
                    z[c, x] = z_new
                    s[c, x] = s_new
                    p[c, x] = p_new
                    r[c, x] = r_new
                    w_later[c, x + 1, LO:HI, :] = w_new
                    ubuf[c, x + 1, LO:HI, :] = ubuf[c, x + 1, LO:HI, :] + alpha * p_new
                    gg = gg + r_new * r_new
                    dd = dd + r_new * w_new
                    held = pack(later, c, x, w_new, held)
                return held, gg, dd

            held, gg, dd = planes(update, (no_pack, nothing, nothing))
            zs[later] = held
            start_sums(later_slot(i), gg, dd)

            @pl.when(i < count - 2)
            def _():
                start_faces(w_later, later, 3)

            return gamma, alpha

        def later_slot(i):
            return lax.rem(i + 1, 2)

        ones = jnp.ones((1, NZL), f32)
        gamma_old, alpha_old = lax.fori_loop(0, count - 1, iterate, (ones, ones))
        slot = (count - 1) % 2
        middle_sums(slot)
        gamma, delta = finish_sums(slot)
        alpha, beta = scalars(count - 1, gamma, delta, gamma_old, alpha_old)

        def last(x, _):
            for c in range(3):
                ubuf[c, x + 1, LO:HI, :] = ubuf[c, x + 1, LO:HI, :] + alpha * (r[c, x] + beta * p[c, x])
            return 0

        planes(last, 0)

    tall = jnp.zeros((NYL, NZL), f32)

    def close(x, carry):
        held, sums = carry
        for c in range(3):
            plane = ubuf[c, x + 1, LO:HI, :]
            vout[c, x] = plane
            held = pack(U_SET, c, x, plane, held)
            if c == 2:
                sums = jnp.where(lane_full == x, jnp.sum(plane, axis=1, keepdims=True), sums)
        return held, sums

    held, sums = planes(close, (no_pack, tall))
    zs[U_SET] = held
    start_faces(ubuf, U_SET, 3)
    square = jnp.concatenate([sums, jnp.zeros((NZL - NYL, NZL), f32)], axis=0)
    across = NZL // NYL
    flat = jnp.transpose(square)[0:NXL]
    tiles[place] = pltpu.roll(flat, lax.rem(my, across) * NYL, 1)

    def tile_copy(k):
        mine = tiles.at[place]
        return pltpu.make_async_remote_copy(
            src_ref=mine, dst_ref=mine, send_sem=tile_send.at[k], recv_sem=tile_recv.at[k],
            device_id=at_group(k), device_id_type=MESH,
        )

    for k in range(1, group):
        tile_copy(k).start()
    finish_faces(ubuf, U_SET, 3)
    u_rim = zr[U_SET]

    def harden(x, _):
        rate = rate_at(x, u_rim)
        plastic = jnp.maximum(rate - strength[x] / (2.0 * visc[x]), 0.0)
        sout[x] = strain[x] + strain_step * plastic
        return 0

    planes(harden, 0)
    for k in range(1, group):
        tile_copy(k).wait()
    scale = surface_step * uplift_gain / (pz * NZL)
    for part in range(py // across):
        total = tiles[part * across * pz]
        for k in range(1, across * pz):
            total = total + tiles[part * across * pz + k]
        span = slice(part * NZL, (part + 1) * NZL)
        tout[:, span] = base[:, span] + scale * total


def build(counts, ident, px, py, pz, name):
    field = (3, NXL, NYL, NZL)
    cell = (NXL, NYL, NZL)
    cols = py * NYL
    group = py * pz
    dma = pltpu.SemaphoreType.DMA
    vmem = pl.BlockSpec(memory_space=pltpu.VMEM)
    return pl.pallas_call(
        functools.partial(step_kernel, counts, px, py, pz),
        out_shape=[
            jax.ShapeDtypeStruct(field, f32),
            jax.ShapeDtypeStruct(cell, f32),
            jax.ShapeDtypeStruct((NXL, cols), f32),
        ],
        in_specs=[vmem] * 7,
        out_specs=[vmem] * 3,
        scratch_shapes=[
            pltpu.VMEM((3, NXL + 2, BUFY, NZL), f32),
            pltpu.VMEM((1, NXL + 2, BUFY, NZL), f32),
            pltpu.VMEM((2, 3, NXL + 2, BUFY, NZL), f32),
            pltpu.VMEM((4, 2, 3, NXL, NZL), f32),
            pltpu.VMEM((4, 2, 3, NXL, NZL), f32),
            pltpu.VMEM((4, NYL // 2, NZL), f32),
            pltpu.VMEM((4, NYL // 2, NZL), f32),
            pltpu.VMEM(cell, f32),
            pltpu.VMEM((7, *cell), f32),
            pltpu.VMEM(field, f32),
            pltpu.VMEM(field, f32),
            pltpu.VMEM(field, f32),
            pltpu.VMEM(field, f32),
            pltpu.VMEM(field, f32),
            pltpu.VMEM((2, px, 2, NZL), f32),
            pltpu.VMEM((2, group, 2, NZL), f32),
            pltpu.VMEM((2, NXL + 2 * RIM, cols), f32),
            pltpu.VMEM((NXL, cols), f32),
            pltpu.VMEM((group, NXL, NZL), f32),
            dma((4, 5)), dma((4, 5)),
            dma((2, px)), dma((2, px)),
            dma((2, group)), dma((2, group)),
            dma((2,)), dma((2,)),
            dma((group,)), dma((group,)),
        ],
        compiler_params=pltpu.CompilerParams(
            collective_id=ident, has_side_effects=True, vmem_limit_bytes=40 * 1024 * 1024
        ),
        name=name,
    )


def local(px, py, pz, force, vel, visc, strain, flags, counts, heights, receivers):
    long_first = build((KMAX, KMAX - 2), 0, px, py, pz, "long_first")
    short_first = build((KMAX - 2, KMAX), 1, px, py, pz, "short_first")
    args = (force, vel, visc, strain, flags, heights, receivers)
    out = lax.cond(counts[0] == KMAX, lambda *a: tuple(long_first(*a)), lambda *a: tuple(short_first(*a)), *args)
    return tuple(out)


def solution(mesh):
    px, py, pz = mesh.shape["mx"], mesh.shape["my"], mesh.shape["mz"]
    vector, scalar, rows = P(None, "mx", "my", "mz"), P("mx", "my", "mz"), P("mx", None)
    return jax.shard_map(
        functools.partial(local, px, py, pz),
        mesh=mesh,
        in_specs=(vector, vector, scalar, scalar, scalar, P(), rows, rows),
        out_specs=(vector, scalar, rows),
        check_vma=False,
    )
```

```python
import functools
import math

import jax
import jax.numpy as jnp
from jax import lax
from jax.experimental import pallas as pl
from jax.experimental.pallas import tpu as pltpu
from jax.sharding import PartitionSpec as P

KMAX = 6
SWEEPS = 4
NXL, NYL, NZL = 16, 32, 128
PADY = 8
LO, HI = PADY, PADY + NYL
BUFY = PADY + NYL + PADY
RIM = 8

drag_coef = 0.05
cohesion_base = 1.0
weakening = 0.6
critical_strain = 1.0
sin_friction = 0.5
cos_friction = 0.8660254
pressure_gradient = 2.0
rate_floor = 0.1
strain_step = 0.5
uplift_gain = 8.0
surface_step = 0.2
erodibility = 0.5
neighbour_steps = ((-1, -1), (-1, 0), (-1, 1), (0, -1), (0, 1), (1, -1), (1, 0), (1, 1))

MESH = pl.DeviceIdType.MESH
U_SET, E_SET = KMAX, KMAX + 1
CUT = 3
ROWS = 32
f32 = jnp.float32


def lanczos(gram, top):
    turn, norms = [], []
    for i in range(top + 1):
        row = [0.0] * i + [1.0]
        for j in range(i):
            part = gram[i, j]
            for k in range(j):
                part = part + turn[j][k] * gram[i, k]
            part = part / norms[j]
            for k in range(j + 1):
                row[k] = row[k] - part * turn[j][k]
        norm = gram[i, i]
        for k in range(i):
            norm = norm + row[k] * gram[i, k]
        turn.append(row)
        norms.append(norm)
    return turn, norms


def solve(gram, shift, n):
    lower, pivots, right = {}, [], []

    def entry(i, j):
        total = gram[i, j + 1]
        for m, part in shift[j].items():
            total = total + part * gram[i, m]
        return total

    for i in range(n):
        for j in range(i):
            part = entry(i, j)
            for k in range(j):
                part = part - lower[i, k] * lower[j, k] * pivots[k]
            lower[i, j] = part / pivots[j]
        pivot = entry(i, i)
        for k in range(i):
            pivot = pivot - lower[i, k] * lower[i, k] * pivots[k]
        pivots.append(pivot)
        part = gram[i, 0]
        for k in range(i):
            part = part - lower[i, k] * right[k]
        right.append(part)
    steps = [part / pivot for part, pivot in zip(right, pivots)]
    for i in reversed(range(n)):
        for k in range(i + 1, n):
            steps[i] = steps[i] - lower[k, i] * steps[k]
    return steps


def step_kernel(
    counts, px, py, pz,
    force, vel, visc, strain, flags, heights, receivers,
    vout, sout, tout,
    ubuf, ebuf, bbuf, ys, yr, zs, zr, strength, coef, dots, sums1, sums2, surf, base, tiles,
    face_send, face_recv, one_send, one_recv, two_send, two_recv, surf_send, surf_recv, tile_send, tile_recv,
):
    mx, my, mz = lax.axis_index("mx"), lax.axis_index("my"), lax.axis_index("mz")
    group = py * pz
    place = my * pz + mz
    edge = (NZL - 1) * (1 - mz)

    def at_group(k):
        other = lax.rem(place + k, group)
        return {"my": other // pz, "mz": lax.rem(other, pz)}

    def at_row(k):
        return {"mx": lax.rem(mx + k, px)}

    def lanes(rows):
        return lax.broadcasted_iota(jnp.int32, (rows, NZL), 1)

    def blank(buf, parts):
        zero = jnp.zeros((NYL, NZL), f32)
        row = jnp.zeros((1, NZL), f32)

        def clear(i, _):
            for c in range(parts):
                buf[c, i, LO - 1 : LO, :] = row
                buf[c, i, HI : HI + 1, :] = row
            return 0

        lax.fori_loop(0, NXL + 2, clear, 0)
        for c in range(parts):
            buf[c, 0, LO:HI, :] = zero
            buf[c, NXL + 1, LO:HI, :] = zero

    blank(ubuf, 3)
    blank(ebuf, 1)
    for k in range(KMAX):
        blank(bbuf.at[k], 3)
    dots[...] = jnp.zeros(dots.shape, f32)
    for kind in range(KMAX + 2):
        for side in range(2):
            for c in range(3):
                yr[kind, side, c] = jnp.zeros((NXL, NZL), f32)
    rows, cols = surf.shape[1:]
    surf[0, 0:RIM, :] = jnp.full((RIM, cols), -1.0, f32)
    surf[0, RIM + NXL :, :] = jnp.full((RIM, cols), -1.0, f32)
    surf[1, 0:RIM, :] = jnp.zeros((RIM, cols), f32)
    surf[1, RIM + NXL :, :] = jnp.zeros((RIM, cols), f32)
    surf[0, RIM : RIM + NXL, :] = receivers[...].astype(f32)
    surf[1, RIM : RIM + NXL, :] = heights[...]

    barrier = pltpu.get_barrier_semaphore()
    for k in range(1, px):
        pl.semaphore_signal(barrier, inc=1, device_id=at_row(k), device_id_type=MESH)
    for k in range(1, group):
        pl.semaphore_signal(barrier, inc=1, device_id=at_group(k), device_id_type=MESH)

    def face_copy(kind, d, src, dst, device):
        return pltpu.make_async_remote_copy(
            src_ref=src, dst_ref=dst, send_sem=face_send.at[kind, d], recv_sem=face_recv.at[kind, d],
            device_id=device, device_id_type=MESH,
        )

    def face_copies(buf, kind, n):
        comps = slice(0, n)
        return (
            (mx < px - 1, mx > 0, 0, buf.at[comps, NXL, LO:HI, :], buf.at[comps, 0, LO:HI, :], {"mx": mx + 1}),
            (mx > 0, mx < px - 1, 1, buf.at[comps, 1, LO:HI, :], buf.at[comps, NXL + 1, LO:HI, :], {"mx": mx - 1}),
            (my < py - 1, my > 0, 2, ys.at[kind, 1, comps], yr.at[kind, 0, comps], {"my": my + 1}),
            (my > 0, my < py - 1, 3, ys.at[kind, 0, comps], yr.at[kind, 1, comps], {"my": my - 1}),
        )

    def depth_copy(kind):
        return face_copy(kind, 4, zs.at[kind], zr.at[kind], {"mz": 1 - mz})

    def start_faces(buf, kind, n):
        depth_copy(kind).start()
        for sends, _, d, src, dst, device in face_copies(buf, kind, n):
            @pl.when(sends)
            def _():
                face_copy(kind, d, src, dst, device).start()

    def finish_faces(buf, kind, n):
        for sends, receives, d, src, dst, device in face_copies(buf, kind, n):
            @pl.when(sends)
            def _():
                face_copy(kind, d, src, dst, device).wait_send()

            @pl.when(receives)
            def _():
                face_copy(kind, d, src, dst, device).wait_recv()
        depth_copy(kind).wait()

    def spread_rows(buf, kind, n):
        for c in range(n):
            low, high = yr[kind, 0, c], yr[kind, 1, c]
            for x in range(NXL):
                buf[c, x + 1, LO - 1 : LO, :] = low[x : x + 1]
                buf[c, x + 1, HI : HI + 1, :] = high[x : x + 1]

    half = NYL // 2
    lane_half = lanes(half)
    lane_full = lanes(NYL)

    def pack(kind, c, x, plane, held):
        ys[kind, 0, c, pl.ds(x, 1), :] = plane[0:1]
        ys[kind, 1, c, pl.ds(x, 1), :] = plane[NYL - 1 :]
        for part in range(2):
            spot = c * NXL + x + 48 * part
            turned = pltpu.roll(plane[part * half : (part + 1) * half], lax.rem(spot - edge + NZL, NZL), 1)
            held = jnp.where(lane_half == spot, turned, held)
        return held

    no_pack = jnp.zeros((half, NZL), f32)

    def depth_pair(v, arrived, c, x):
        parts = []
        for part in range(2):
            spot = c * NXL + x + 48 * part
            parts.append(pltpu.roll(arrived, lax.rem(edge - spot + NZL, NZL), 1))
        rim = jnp.where(lane_full == edge, jnp.concatenate(parts, axis=0), 0.0)
        below = jnp.where(lane_full == 0, rim, pltpu.roll(v, 1, 1))
        above = jnp.where(lane_full == NZL - 1, rim, pltpu.roll(v, NZL - 1, 1))
        return below, above

    def around(buf, arrived, c, x):
        v = buf[c, x + 1, LO:HI, :]
        below, above = depth_pair(v, arrived, c, x)
        return v, (
            (buf[c, x, LO:HI, :], buf[c, x + 2, LO:HI, :]),
            (buf[c, x + 1, LO - 1 : HI - 1, :], buf[c, x + 1, LO + 1 : HI + 1, :]),
            (below, above),
        )

    def applied(buf, arrived, c, x):
        v, pairs = around(buf, arrived, c, x)
        total = coef[6, x] * v
        for d in range(3):
            total = total - coef[2 * d, x] * pairs[d][0] - coef[2 * d + 1, x] * pairs[d][1]
        return v, total

    def rate_at(x, arrived):
        g = []
        for c in range(3):
            _, pairs = around(ubuf, arrived, c, x)
            g.append([0.5 * (pair[1] - pair[0]) for pair in pairs])
        total = g[0][0] * g[0][0] + g[1][1] * g[1][1] + g[2][2] * g[2][2]
        for a, b in ((0, 1), (0, 2), (1, 2)):
            shear = g[a][b] + g[b][a]
            total = total + 0.5 * (shear * shear)
        return jnp.sqrt(0.5 * total)

    def planes(body, carry, unroll=2):
        return lax.fori_loop(0, NXL, body, carry, unroll=unroll)

    def one_copy(slot, k):
        mine = sums1.at[slot, mx]
        return pltpu.make_async_remote_copy(
            src_ref=mine, dst_ref=mine, send_sem=one_send.at[slot, k], recv_sem=one_recv.at[slot, k],
            device_id=at_row(k), device_id_type=MESH,
        )

    def two_copy(slot, k):
        mine = sums2.at[slot, place]
        return pltpu.make_async_remote_copy(
            src_ref=mine, dst_ref=mine, send_sem=two_send.at[slot, k], recv_sem=two_recv.at[slot, k],
            device_id=at_group(k), device_id_type=MESH,
        )

    def start_sums(slot, bank):
        spot = lax.broadcasted_iota(jnp.int32, (ROWS, NZL), 0) == lanes(ROWS)
        line = jnp.sum(dots[bank], axis=1, keepdims=True)
        sums1[slot, mx] = jnp.sum(jnp.where(spot, line, 0.0), axis=0, keepdims=True)
        for k in range(1, px):
            one_copy(slot, k).start()

    def middle_sums(slot):
        for k in range(1, px):
            one_copy(slot, k).wait()
        sums2[slot, place] = jnp.sum(sums1[slot], axis=0)
        for k in range(1, group):
            two_copy(slot, k).start()

    def finish_sums(slot, names, gram):
        for k in range(1, group):
            two_copy(slot, k).wait()
        total = jnp.sum(sums2[slot], axis=0)
        for spot, (i, j) in enumerate(names):
            gram[i, j] = gram[j, i] = jnp.broadcast_to(total[:, spot : spot + 1], (1, NZL))

    def fold(product):
        return (product[0:8] + product[8:16]) + (product[16:24] + product[24:32])

    def keep_dots(bank, names, pairs, sums):
        for pair, total in zip(pairs, sums):
            spot = len(names)
            dots[bank, spot : spot + 1, :] = jnp.sum(total, axis=0, keepdims=True)
            names.append(pair)

    def straighten(mix, names):
        pairs = [(m, CUT) for m in range(CUT + 1)]
        for rim_of in (0, NXL + 1):
            for c in range(3):
                plane = bbuf[CUT, c, rim_of, LO:HI, :]
                for m in range(CUT):
                    plane = plane - mix[m] * bbuf[m, c, rim_of, LO:HI, :]
                bbuf[CUT, c, rim_of, LO:HI, :] = plane
        for side in range(2):
            for c in range(3):
                face = yr[CUT, side, c]
                for m in range(CUT):
                    face = face - mix[m] * yr[m, side, c]
                yr[CUT, side, c] = face
        face = zr[CUT]
        for m in range(CUT):
            face = face - mix[m] * zr[m]
        zr[CUT] = face

        def one(x, sums):
            sums = list(sums)
            for c in range(3):
                own = [bbuf[m, c, x + 1, LO:HI, :] for m in range(CUT)]
                plane = bbuf[CUT, c, x + 1, LO:HI, :]
                for m in range(CUT):
                    plane = plane - mix[m] * own[m]
                bbuf[CUT, c, x + 1, LO:HI, :] = plane
                own.append(plane)
                for m in range(CUT + 1):
                    sums[m] = sums[m] + fold(own[m] * plane)
            return tuple(sums)

        sums = planes(one, tuple(jnp.zeros((8, NZL), f32) for _ in range(CUT + 1)))
        keep_dots(1, names, pairs, sums)

    def load(x, held):
        for c in range(3):
            plane = vel[c, x]
            ubuf[c, x + 1, LO:HI, :] = plane
            held = pack(U_SET, c, x, plane, held)
        return held

    zs[U_SET] = planes(load, no_pack)
    pl.semaphore_wait(barrier, px - 1 + group - 1)
    start_faces(ubuf, U_SET, 3)

    def surf_copy(d):
        if d == 0:
            src, dst, device = surf.at[:, NXL : NXL + RIM], surf.at[:, 0:RIM], {"mx": mx + 1}
        else:
            src, dst, device = surf.at[:, RIM : 2 * RIM], surf.at[:, RIM + NXL : RIM + NXL + RIM], {"mx": mx - 1}
        return pltpu.make_async_remote_copy(
            src_ref=src, dst_ref=dst, send_sem=surf_send.at[d], recv_sem=surf_recv.at[d],
            device_id=device, device_id_type=MESH,
        )

    for d, sends in ((0, mx < px - 1), (1, mx > 0)):
        @pl.when(sends)
        def _():
            surf_copy(d).start()

    depth_at = mz * NZL + lane_full
    pressure = pressure_gradient * (pz * NZL - 0.5 - depth_at.astype(f32)) / (pz * NZL)

    def strengthen(x, _):
        weak = flags[x].astype(f32) * jnp.minimum(strain[x] / critical_strain, 1.0)
        strength[x] = cohesion_base * (1.0 - weakening * weak) * cos_friction + pressure * sin_friction
        return 0

    planes(strengthen, 0)

    for d, sends, receives in ((0, mx < px - 1, mx > 0), (1, mx > 0, mx < px - 1)):
        @pl.when(sends)
        def _():
            surf_copy(d).wait_send()

        @pl.when(receives)
        def _():
            surf_copy(d).wait_recv()

    code = surf[0]
    col = lax.broadcasted_iota(jnp.int32, (rows, cols), 1)

    def turned(block, row_step, col_step):
        if col_step:
            block = pltpu.roll(block, col_step % cols, 1)
        if row_step:
            block = pltpu.roll(block, row_step % rows, 0)
        return block

    drained = jnp.ones((rows, cols), f32)
    for _ in range(SWEEPS):
        total = jnp.ones((rows, cols), f32)
        for direction, (row_step, col_step) in enumerate(neighbour_steps):
            chosen = code == float(direction)
            if col_step:
                chosen = chosen & (col != (cols - 1 if col_step > 0 else 0))
            total = total + turned(jnp.where(chosen, drained, 0.0), row_step, col_step)
        drained = total
    height = surf[1]
    below = jnp.zeros((rows, cols), f32)
    spacing = jnp.ones((rows, cols), f32)
    for direction, (row_step, col_step) in enumerate(neighbour_steps):
        chosen = code == float(direction)
        seen = chosen
        if col_step:
            seen = seen & (col != (cols - 1 if col_step > 0 else 0))
        below = below + jnp.where(seen, turned(height, -row_step, -col_step), 0.0)
        if row_step and col_step:
            spacing = jnp.where(chosen, math.sqrt(2.0), spacing)
    slope = jnp.maximum(height - below, 0.0) / spacing
    ground = height - (surface_step * erodibility) * jnp.sqrt(drained) * slope
    base[...] = ground[RIM : RIM + NXL]

    none = jnp.zeros((8, NZL), f32)
    finish_faces(ubuf, U_SET, 3)
    spread_rows(ubuf, U_SET, 3)
    for picard, count in enumerate(counts):
        u_rim = zr[U_SET]

        def soften(x, held):
            rate = rate_at(x, u_rim)
            eta = jnp.minimum(visc[x], strength[x] / (2.0 * jnp.maximum(rate, rate_floor)))
            ebuf[0, x + 1, LO:HI, :] = eta
            return pack(E_SET, 0, x, eta, held)

        zs[E_SET] = planes(soften, no_pack)
        start_faces(ebuf, E_SET, 1)
        finish_faces(ebuf, E_SET, 1)
        spread_rows(ebuf, E_SET, 1)
        e_rim = zr[E_SET]
        lagged = count <= CUT + 1
        gram, rows_of = {}, ([], [])
        shift = {}

        def begin(x, carry):
            held, norm = carry
            eta, pairs = around(ebuf, e_rim, 0, x)
            total = jnp.full((NYL, NZL), drag_coef, f32)
            for d in range(3):
                for side in range(2):
                    face = 0.5 * (eta + pairs[d][side])
                    coef[2 * d + side, x] = face
                    total = total + face
            coef[6, x] = total
            for c in range(3):
                _, au = applied(ubuf, u_rim, c, x)
                plane = force[c, x] - au
                bbuf[0, c, x + 1, LO:HI, :] = plane
                norm = norm + fold(plane * plane)
                held = pack(0, c, x, plane, held)
            return held, norm

        held, norm = planes(begin, (no_pack, none), 1)
        zs[0] = held
        keep_dots(0, rows_of[0], [(0, 0)], [norm])
        start_faces(bbuf.at[0], 0, 3)
        early = 2 * picard
        for k in range(count):
            if k != CUT:
                finish_faces(bbuf.at[k], k, 3)
                spread_rows(bbuf.at[k], k, 3)
            if lagged and k == CUT - 1:
                middle_sums(early)
            rim = zr[k]
            stored = k + 1 < count
            extra = {}
            if k >= CUT:
                extra[k] = alpha
                if k == CUT:
                    for m in range(CUT):
                        extra[m] = beta * turn[CUT - 1][m]
                else:
                    extra[k - 1] = beta
            partners = [m for m in range(k + 2 if stored else k + 1)]
            if k + 1 == CUT and lagged:
                partners = []

            def grow(x, carry):
                held, sums = carry
                sums = list(sums)
                for c in range(3):
                    v, w = applied(bbuf.at[k], rim, c, x)
                    own = {}
                    for m in set(extra) | set(partners):
                        if m <= k:
                            own[m] = v if m == k else bbuf[m, c, x + 1, LO:HI, :]
                    for m in sorted(extra):
                        w = w - extra[m] * own[m]
                    own[k + 1] = w
                    if stored:
                        bbuf[k + 1, c, x + 1, LO:HI, :] = w
                        held = pack(k + 1, c, x, w, held)
                    for at, m in enumerate(partners):
                        sums[at] = sums[at] + fold(own[m] * w)
                return held, tuple(sums)

            held, sums = planes(grow, (no_pack, tuple(none for _ in partners)))
            shift[k] = dict(extra)
            bank = 0 if k + 1 < CUT or (k + 1 == CUT and not lagged) else 1
            keep_dots(bank, rows_of[bank], [(m, k + 1) for m in partners], sums)
            if k + 1 == (CUT - 1 if lagged else CUT):
                start_sums(early, 0)
            if stored:
                zs[k + 1] = held
                start_faces(bbuf.at[k + 1], k + 1, 3)
            if k + 1 == CUT:
                if not lagged:
                    middle_sums(early)
                finish_faces(bbuf.at[CUT], CUT, 3)
                finish_sums(early, rows_of[0], gram)
                turn, norms = lanczos(gram, CUT - 1 if lagged else CUT)
                top = CUT - 1 if lagged else CUT
                beta = norms[top] / norms[top - 1]
                alpha = turn[top - 1][top - 2] - turn[top][top - 1]
                if lagged:
                    full = [0.0] * (CUT + 1)
                    for m in range(CUT):
                        full[m + 1] = full[m + 1] + turn[top][m]
                        full[m] = full[m] - alpha * turn[top][m]
                    for m in range(CUT - 1):
                        full[m] = full[m] - beta * turn[top - 1][m]
                    mix = [-full[m] for m in range(CUT)]
                else:
                    mix = [-turn[CUT][m] for m in range(CUT)]
                shift[CUT - 1] = dict(enumerate(mix))
                straighten(mix, rows_of[1])
                spread_rows(bbuf.at[CUT], CUT, 3)

        start_sums(early + 1, 1)
        middle_sums(early + 1)
        finish_sums(early + 1, rows_of[1], gram)
        steps = solve(gram, shift, count)
        final = picard == len(counts) - 1
        tall = jnp.zeros((NYL, NZL), f32)

        def total_of(first, parts):
            for step, part in zip(steps, parts):
                first = first + step * part
            return first

        for rim_of in (0, NXL + 1):
            for c in range(3):
                ubuf[c, rim_of, LO:HI, :] = total_of(
                    ubuf[c, rim_of, LO:HI, :], [bbuf[m, c, rim_of, LO:HI, :] for m in range(count)]
                )
        for side in range(2):
            for c in range(3):
                yr[U_SET, side, c] = total_of(yr[U_SET, side, c], [yr[m, side, c] for m in range(count)])
        zr[U_SET] = total_of(zr[U_SET], [zr[m] for m in range(count)])

        def settle(x, sums):
            for c in range(3):
                plane = total_of(
                    ubuf[c, x + 1, LO:HI, :], [bbuf[m, c, x + 1, LO:HI, :] for m in range(count)]
                )
                ubuf[c, x + 1, LO:HI, :] = plane
                if final:
                    vout[c, x] = plane
                    if c == 2:
                        sums = jnp.where(lane_full == x, jnp.sum(plane, axis=1, keepdims=True), sums)
            return sums

        sums = planes(settle, tall)
        spread_rows(ubuf, U_SET, 3)

    square = jnp.concatenate([sums, jnp.zeros((NZL - NYL, NZL), f32)], axis=0)
    across = NZL // NYL
    flat = jnp.transpose(square)[0:NXL]
    tiles[place] = pltpu.roll(flat, lax.rem(my, across) * NYL, 1)

    def tile_copy(k):
        mine = tiles.at[place]
        return pltpu.make_async_remote_copy(
            src_ref=mine, dst_ref=mine, send_sem=tile_send.at[k], recv_sem=tile_recv.at[k],
            device_id=at_group(k), device_id_type=MESH,
        )

    for k in range(1, group):
        tile_copy(k).start()
    u_rim = zr[U_SET]

    def harden(x, _):
        rate = rate_at(x, u_rim)
        plastic = jnp.maximum(rate - strength[x] / (2.0 * visc[x]), 0.0)
        sout[x] = strain[x] + strain_step * plastic
        return 0

    planes(harden, 0)
    for k in range(1, group):
        tile_copy(k).wait()
    scale = surface_step * uplift_gain / (pz * NZL)
    for part in range(py // across):
        total = tiles[part * across * pz]
        for k in range(1, across * pz):
            total = total + tiles[part * across * pz + k]
        span = slice(part * NZL, (part + 1) * NZL)
        tout[:, span] = base[:, span] + scale * total


def build(counts, ident, px, py, pz, name):
    field = (3, NXL, NYL, NZL)
    cell = (NXL, NYL, NZL)
    cols = py * NYL
    group = py * pz
    dma = pltpu.SemaphoreType.DMA
    vmem = pl.BlockSpec(memory_space=pltpu.VMEM)
    return pl.pallas_call(
        functools.partial(step_kernel, counts, px, py, pz),
        out_shape=[
            jax.ShapeDtypeStruct(field, f32),
            jax.ShapeDtypeStruct(cell, f32),
            jax.ShapeDtypeStruct((NXL, cols), f32),
        ],
        in_specs=[vmem] * 7,
        out_specs=[vmem] * 3,
        scratch_shapes=[
            pltpu.VMEM((3, NXL + 2, BUFY, NZL), f32),
            pltpu.VMEM((1, NXL + 2, BUFY, NZL), f32),
            pltpu.VMEM((KMAX, 3, NXL + 2, BUFY, NZL), f32),
            pltpu.VMEM((KMAX + 2, 2, 3, NXL, NZL), f32),
            pltpu.VMEM((KMAX + 2, 2, 3, NXL, NZL), f32),
            pltpu.VMEM((KMAX + 2, NYL // 2, NZL), f32),
            pltpu.VMEM((KMAX + 2, NYL // 2, NZL), f32),
            pltpu.VMEM(cell, f32),
            pltpu.VMEM((7, *cell), f32),
            pltpu.VMEM((2, ROWS, NZL), f32),
            pltpu.VMEM((4, px, 1, NZL), f32),
            pltpu.VMEM((4, group, 1, NZL), f32),
            pltpu.VMEM((2, NXL + 2 * RIM, cols), f32),
            pltpu.VMEM((NXL, cols), f32),
            pltpu.VMEM((group, NXL, NZL), f32),
            dma((KMAX + 2, 5)), dma((KMAX + 2, 5)),
            dma((4, px)), dma((4, px)),
            dma((4, group)), dma((4, group)),
            dma((2,)), dma((2,)),
            dma((group,)), dma((group,)),
        ],
        compiler_params=pltpu.CompilerParams(
            collective_id=ident, has_side_effects=True, vmem_limit_bytes=40 * 1024 * 1024
        ),
        name=name,
    )


def local(px, py, pz, force, vel, visc, strain, flags, counts, heights, receivers):
    long_first = build((KMAX, KMAX - 2), 0, px, py, pz, "long_first")
    short_first = build((KMAX - 2, KMAX), 1, px, py, pz, "short_first")
    args = (force, vel, visc, strain, flags, heights, receivers)
    out = lax.cond(counts[0] == KMAX, lambda *a: tuple(long_first(*a)), lambda *a: tuple(short_first(*a)), *args)
    return tuple(out)


def solution(mesh):
    px, py, pz = mesh.shape["mx"], mesh.shape["my"], mesh.shape["mz"]
    vector, scalar, rows = P(None, "mx", "my", "mz"), P("mx", "my", "mz"), P("mx", None)
    return jax.shard_map(
        functools.partial(local, px, py, pz),
        mesh=mesh,
        in_specs=(vector, vector, scalar, scalar, scalar, P(), rows, rows),
        out_specs=(vector, scalar, rows),
        check_vma=False,
    )
```

```python
import functools
import math

import jax
import jax.numpy as jnp
from jax import lax
from jax.experimental import pallas as pl
from jax.experimental.pallas import tpu as pltpu
from jax.sharding import PartitionSpec as P

KMAX = 6
SWEEPS = 4
NXL, NYL, NZL = 16, 32, 128
PADY = 8
LO, HI = PADY, PADY + NYL
BUFY = PADY + NYL + PADY
RIM = 8

drag_coef = 0.05
cohesion_base = 1.0
weakening = 0.6
critical_strain = 1.0
sin_friction = 0.5
cos_friction = 0.8660254
pressure_gradient = 2.0
rate_floor = 0.1
strain_step = 0.5
uplift_gain = 8.0
surface_step = 0.2
erodibility = 0.5
neighbour_steps = ((-1, -1), (-1, 0), (-1, 1), (0, -1), (0, 1), (1, -1), (1, 0), (1, 1))

MESH = pl.DeviceIdType.MESH
U_SET, E_SET = KMAX, KMAX + 1
CUT = 3
ROWS = 32
f32 = jnp.float32


def lanczos(gram, top):
    turn, norms = [], []
    for i in range(top + 1):
        row = [0.0] * i + [1.0]
        for j in range(i):
            part = gram[i, j]
            for k in range(j):
                part = part + turn[j][k] * gram[i, k]
            part = part / norms[j]
            for k in range(j + 1):
                row[k] = row[k] - part * turn[j][k]
        norm = gram[i, i]
        for k in range(i):
            norm = norm + row[k] * gram[i, k]
        turn.append(row)
        norms.append(norm)
    return turn, norms


def solve(gram, shift, n):
    lower, pivots, right = {}, [], []

    def entry(i, j):
        total = gram[i, j + 1]
        for m, part in shift[j].items():
            total = total + part * gram[i, m]
        return total

    for i in range(n):
        for j in range(i):
            part = entry(i, j)
            for k in range(j):
                part = part - lower[i, k] * lower[j, k] * pivots[k]
            lower[i, j] = part / pivots[j]
        pivot = entry(i, i)
        for k in range(i):
            pivot = pivot - lower[i, k] * lower[i, k] * pivots[k]
        pivots.append(pivot)
        part = gram[i, 0]
        for k in range(i):
            part = part - lower[i, k] * right[k]
        right.append(part)
    steps = [part / pivot for part, pivot in zip(right, pivots)]
    for i in reversed(range(n)):
        for k in range(i + 1, n):
            steps[i] = steps[i] - lower[k, i] * steps[k]
    return steps


def step_kernel(
    counts, px, py, pz,
    force_in, vel_in, visc_in, strain_in, flags_in, heights_in, receivers_in,
    vout, sout, tout,
    force, visc, strain, flags, heights, receivers, load_sem,
    ubuf, ebuf, bbuf, ys, yr, zs, zr, strength, coef, dots, sums1, sums2, surf, base, tiles,
    face_send, face_recv, one_send, one_recv, two_send, two_recv, surf_send, surf_recv, tile_send, tile_recv,
):
    mx, my, mz = lax.axis_index("mx"), lax.axis_index("my"), lax.axis_index("mz")
    group = py * pz
    place = my * pz + mz
    edge = (NZL - 1) * (1 - mz)

    def at_group(k):
        other = lax.rem(place + k, group)
        return {"my": other // pz, "mz": lax.rem(other, pz)}

    def at_row(k):
        return {"mx": lax.rem(mx + k, px)}

    def lanes(rows):
        return lax.broadcasted_iota(jnp.int32, (rows, NZL), 1)

    def blank(buf, parts):
        zero = jnp.zeros((NYL, NZL), f32)
        row = jnp.zeros((1, NZL), f32)

        def clear(i, _):
            for c in range(parts):
                buf[c, i, LO - 1 : LO, :] = row
                buf[c, i, HI : HI + 1, :] = row
            return 0

        lax.fori_loop(0, NXL + 2, clear, 0)
        for c in range(parts):
            buf[c, 0, LO:HI, :] = zero
            buf[c, NXL + 1, LO:HI, :] = zero

    loads = [
        pltpu.make_async_copy(src, dst, load_sem.at[k])
        for k, (src, dst) in enumerate((
            (vel_in, ubuf.at[:, 1 : NXL + 1, LO:HI, :]), (heights_in, heights), (receivers_in, receivers),
            (strain_in, strain), (flags_in, flags), (visc_in, visc), (force_in, force),
        ))
    ]
    for copy in loads:
        copy.start()

    blank(ubuf, 3)
    blank(ebuf, 1)

    def blank_one(k, _):
        blank(bbuf.at[k], 3)
        return 0

    lax.fori_loop(0, KMAX, blank_one, 0)
    dots[...] = jnp.zeros(dots.shape, f32)

    def blank_rows(kind, _):
        for side in range(2):
            for c in range(3):
                yr[kind, side, c] = jnp.zeros((NXL, NZL), f32)
        return 0

    lax.fori_loop(0, KMAX + 2, blank_rows, 0)
    rows, cols = surf.shape[1:]
    surf[0, 0:RIM, :] = jnp.full((RIM, cols), -1.0, f32)
    surf[0, RIM + NXL :, :] = jnp.full((RIM, cols), -1.0, f32)
    surf[1, 0:RIM, :] = jnp.zeros((RIM, cols), f32)
    surf[1, RIM + NXL :, :] = jnp.zeros((RIM, cols), f32)

    barrier = pltpu.get_barrier_semaphore()
    for k in range(1, px):
        pl.semaphore_signal(barrier, inc=1, device_id=at_row(k), device_id_type=MESH)
    for k in range(1, group):
        pl.semaphore_signal(barrier, inc=1, device_id=at_group(k), device_id_type=MESH)

    turn_of = {"start": 0, "finish": 0}

    def face_copy(turn, d, src, dst, device):
        return pltpu.make_async_remote_copy(
            src_ref=src, dst_ref=dst, send_sem=face_send.at[d], recv_sem=face_recv.at[turn, d],
            device_id=device, device_id_type=MESH,
        )

    def face_copies(buf, kind, n):
        comps = slice(0, n)
        return (
            (mx < px - 1, mx > 0, 0, buf.at[comps, NXL, LO:HI, :], buf.at[comps, 0, LO:HI, :], {"mx": mx + 1}),
            (mx > 0, mx < px - 1, 1, buf.at[comps, 1, LO:HI, :], buf.at[comps, NXL + 1, LO:HI, :], {"mx": mx - 1}),
            (my < py - 1, my > 0, 2, ys.at[kind, 1, comps], yr.at[kind, 0, comps], {"my": my + 1}),
            (my > 0, my < py - 1, 3, ys.at[kind, 0, comps], yr.at[kind, 1, comps], {"my": my - 1}),
        )

    def depth_copy(turn, kind):
        return face_copy(turn, 4, zs.at[kind], zr.at[kind], {"mz": 1 - mz})

    def start_faces(buf, kind, n):
        turn = turn_of["start"] % 2
        turn_of["start"] += 1
        depth_copy(turn, kind).start()
        for sends, _, d, src, dst, device in face_copies(buf, kind, n):
            @pl.when(sends)
            def _():
                face_copy(turn, d, src, dst, device).start()

    def finish_faces(buf, kind, n):
        turn = turn_of["finish"] % 2
        turn_of["finish"] += 1
        for sends, receives, d, src, dst, device in face_copies(buf, kind, n):
            @pl.when(sends)
            def _():
                face_copy(turn, d, src, dst, device).wait_send()

            @pl.when(receives)
            def _():
                face_copy(turn, d, src, dst, device).wait_recv()
        depth_copy(turn, kind).wait()

    def spread_rows(buf, kind, n):
        def spread(x, _):
            for c in range(n):
                buf[c, x + 1, LO - 1 : LO, :] = yr[kind, 0, c, pl.ds(x, 1), :]
                buf[c, x + 1, HI : HI + 1, :] = yr[kind, 1, c, pl.ds(x, 1), :]
            return 0

        lax.fori_loop(0, NXL, spread, 0, unroll=4)

    lane_full = lanes(NYL)
    lane_tile = lanes(8)
    tiles_in = range(NYL // 8)

    def at(t, step=0):
        return slice(LO + 8 * t + step, LO + 8 * t + step + 8)

    def own(t):
        return slice(8 * t, 8 * t + 8)

    def pack(kind, c, x, t, tile, held):
        if t == 0:
            ys[kind, 0, c, pl.ds(x, 1), :] = tile[0:1]
        if t == NYL // 8 - 1:
            ys[kind, 1, c, pl.ds(x, 1), :] = tile[7:8]
        spot = c * NXL + x + 48 * (t // 2)
        turned = pltpu.roll(tile, spot - edge + NZL, 1)
        held = list(held)
        held[t % 2] = jnp.where(lane_tile == spot, turned, held[t % 2])
        return tuple(held)

    none = jnp.zeros((8, NZL), f32)
    no_pack = (none, none)

    def keep_pack(kind, held):
        zs[kind, 0:8] = held[0]
        zs[kind, 8:16] = held[1]

    def turned_rim(kind, c, x, t):
        spot = c * NXL + x + 48 * (t // 2)
        return pltpu.roll(zr[kind, own(t % 2)], edge - spot + NZL, 1)

    def around(buf, kind, c, x, t):
        v = buf[c, x + 1, at(t), :]
        rim = jnp.where(lane_tile == edge, turned_rim(kind, c, x, t), 0.0)
        below = jnp.where(lane_tile == 0, rim, pltpu.roll(v, 1, 1))
        above = jnp.where(lane_tile == NZL - 1, rim, pltpu.roll(v, NZL - 1, 1))
        return v, (
            (buf[c, x, at(t), :], buf[c, x + 2, at(t), :]),
            (buf[c, x + 1, at(t, -1), :], buf[c, x + 1, at(t, 1), :]),
            (below, above),
        )

    def applied(buf, kind, c, x, t):
        v = buf[c, x + 1, at(t), :]
        total = coef[6, x, own(t)] * v
        total = total - coef[0, x, own(t)] * buf[c, x, at(t), :] - coef[1, x, own(t)] * buf[c, x + 2, at(t), :]
        total = total - coef[2, x, own(t)] * buf[c, x + 1, at(t, -1), :]
        total = total - coef[3, x, own(t)] * buf[c, x + 1, at(t, 1), :]
        total = total - coef[4, x, own(t)] * pltpu.roll(v, 1, 1) - coef[5, x, own(t)] * pltpu.roll(v, NZL - 1, 1)
        return v, total - coef[7, x, own(t)] * turned_rim(kind, c, x, t)

    def rate_at(x, t):
        g = []
        for c in range(3):
            _, pairs = around(ubuf, U_SET, c, x, t)
            g.append([0.5 * (pair[1] - pair[0]) for pair in pairs])
        total = g[0][0] * g[0][0] + g[1][1] * g[1][1] + g[2][2] * g[2][2]
        for a, b in ((0, 1), (0, 2), (1, 2)):
            shear = g[a][b] + g[b][a]
            total = total + 0.5 * (shear * shear)
        return jnp.sqrt(0.5 * total)

    def planes(body, carry, unroll=2):
        return lax.fori_loop(0, NXL, body, carry, unroll=unroll)

    def sum_copy(sums, slot, mine, send, recv, device):
        ref = sums.at[slot, mine]
        return pltpu.make_async_remote_copy(
            src_ref=ref, dst_ref=ref, send_sem=send, recv_sem=recv, device_id=device, device_id_type=MESH
        )

    def one_copy(slot, mine, k):
        return sum_copy(sums1, slot, mine, one_send.at[0], one_recv.at[slot % 2], at_row(k))

    def two_copy(slot, mine, k):
        return sum_copy(sums2, slot, mine, two_send.at[0], two_recv.at[slot % 2], at_group(k))

    def start_sums(slot, bank):
        spot = lax.broadcasted_iota(jnp.int32, (ROWS, NZL), 0) == lanes(ROWS)
        line = jnp.sum(dots[bank], axis=1, keepdims=True)
        sums1[slot, mx] = jnp.sum(jnp.where(spot, line, 0.0), axis=0, keepdims=True)
        for k in range(1, px):
            one_copy(slot, mx, k).start()

    def middle_sums(slot):
        one_copy(slot, slice(0, px - 1), 1).wait()
        sums2[slot, place] = jnp.sum(sums1[slot], axis=0)
        for k in range(1, group):
            two_copy(slot, place, k).start()

    def finish_sums(slot, names, gram):
        two_copy(slot, slice(0, group - 1), 1).wait()
        total = jnp.sum(sums2[slot], axis=0)
        for spot, (i, j) in enumerate(names):
            gram[i, j] = gram[j, i] = jnp.broadcast_to(total[:, spot : spot + 1], (1, NZL))

    def keep_dots(bank, names, pairs, sums):
        for pair, total in zip(pairs, sums):
            spot = len(names)
            dots[bank, spot : spot + 1, :] = jnp.sum(total, axis=0, keepdims=True)
            names.append(pair)

    def straighten(mix, names):
        pairs = [(m, CUT) for m in range(CUT + 1)]
        for rim_of in (0, NXL + 1):
            for c in range(3):
                plane = bbuf[CUT, c, rim_of, LO:HI, :]
                for m in range(CUT):
                    plane = plane - mix[m] * bbuf[m, c, rim_of, LO:HI, :]
                bbuf[CUT, c, rim_of, LO:HI, :] = plane
        for side in range(2):
            for c in range(3):
                face = yr[CUT, side, c]
                for m in range(CUT):
                    face = face - mix[m] * yr[m, side, c]
                yr[CUT, side, c] = face
        face = zr[CUT]
        for m in range(CUT):
            face = face - mix[m] * zr[m]
        zr[CUT] = face

        def one(x, sums):
            sums = list(sums)
            for t in tiles_in:
                for c in range(3):
                    mine = [bbuf[m, c, x + 1, at(t), :] for m in range(CUT)]
                    tile = bbuf[CUT, c, x + 1, at(t), :]
                    for m in range(CUT):
                        tile = tile - mix[m] * mine[m]
                    bbuf[CUT, c, x + 1, at(t), :] = tile
                    mine.append(tile)
                    for m in range(CUT + 1):
                        sums[m] = sums[m] + mine[m] * tile
            return tuple(sums)

        sums = planes(one, (none,) * (CUT + 1))
        keep_dots(1, names, pairs, sums)

    across = NZL // NYL

    def tile_copy(mine, k):
        ref = tiles.at[mine]
        return pltpu.make_async_remote_copy(
            src_ref=ref, dst_ref=ref, send_sem=tile_send.at[0], recv_sem=tile_recv.at[0],
            device_id=at_group(k), device_id_type=MESH,
        )

    def send_depth_sums(count):
        tall = jnp.zeros((NYL, NZL), f32)

        def add_up(x, sums):
            fields = [ubuf[2, x + 1, LO:HI, :]] + [bbuf[m, 2, x + 1, LO:HI, :] for m in range(count)]
            return tuple(
                jnp.where(lane_full == x, jnp.sum(plane, axis=1, keepdims=True), old)
                for plane, old in zip(fields, sums)
            )

        sums = list(planes(add_up, (tall,) * (count + 1), 1)) + [tall] * (2 * across - count - 1)
        for t in range(2):
            square = jnp.concatenate(sums[t * across : (t + 1) * across], axis=0)
            tiles[place, t] = jnp.transpose(square)[0:NXL]
        for k in range(1, group):
            tile_copy(place, k).start()

    def load(x, held):
        for c in range(3):
            for t in tiles_in:
                held = pack(U_SET, c, x, t, ubuf[c, x + 1, at(t), :], held)
        return held

    loads[0].wait()
    keep_pack(U_SET, planes(load, no_pack))
    pl.semaphore_wait(barrier, px - 1 + group - 1)
    start_faces(ubuf, U_SET, 3)

    def surf_copy(d):
        if d == 0:
            src, dst, device = surf.at[:, NXL : NXL + RIM], surf.at[:, 0:RIM], {"mx": mx + 1}
        else:
            src, dst, device = surf.at[:, RIM : 2 * RIM], surf.at[:, RIM + NXL : RIM + NXL + RIM], {"mx": mx - 1}
        return pltpu.make_async_remote_copy(
            src_ref=src, dst_ref=dst, send_sem=surf_send.at[d], recv_sem=surf_recv.at[d],
            device_id=device, device_id_type=MESH,
        )

    for copy in loads[1:]:
        copy.wait()
    surf[0, RIM : RIM + NXL, :] = receivers[...].astype(f32)
    surf[1, RIM : RIM + NXL, :] = heights[...]
    for d, sends in ((0, mx < px - 1), (1, mx > 0)):
        @pl.when(sends)
        def _():
            surf_copy(d).start()

    depth_at = mz * NZL + lane_full
    pressure = pressure_gradient * (pz * NZL - 0.5 - depth_at.astype(f32)) / (pz * NZL)

    def strengthen(x, _):
        weak = flags[x].astype(f32) * jnp.minimum(strain[x] / critical_strain, 1.0)
        strength[x] = cohesion_base * (1.0 - weakening * weak) * cos_friction + pressure * sin_friction
        return 0

    planes(strengthen, 0)

    for d, sends, receives in ((0, mx < px - 1, mx > 0), (1, mx > 0, mx < px - 1)):
        @pl.when(sends)
        def _():
            surf_copy(d).wait_send()

        @pl.when(receives)
        def _():
            surf_copy(d).wait_recv()

    code = surf[0]
    col = lax.broadcasted_iota(jnp.int32, (rows, cols), 1)

    def turned(block, row_step, col_step):
        if col_step:
            block = pltpu.roll(block, col_step % cols, 1)
        if row_step:
            block = pltpu.roll(block, row_step % rows, 0)
        return block

    def sweep(_, drained):
        total = jnp.ones((rows, cols), f32)
        for direction, (row_step, col_step) in enumerate(neighbour_steps):
            chosen = code == float(direction)
            if col_step:
                chosen = chosen & (col != (cols - 1 if col_step > 0 else 0))
            total = total + turned(jnp.where(chosen, drained, 0.0), row_step, col_step)
        return total

    drained = lax.fori_loop(0, SWEEPS, sweep, jnp.ones((rows, cols), f32))
    height = surf[1]
    below = jnp.zeros((rows, cols), f32)
    spacing = jnp.ones((rows, cols), f32)
    for direction, (row_step, col_step) in enumerate(neighbour_steps):
        chosen = code == float(direction)
        seen = chosen
        if col_step:
            seen = seen & (col != (cols - 1 if col_step > 0 else 0))
        below = below + jnp.where(seen, turned(height, -row_step, -col_step), 0.0)
        if row_step and col_step:
            spacing = jnp.where(chosen, math.sqrt(2.0), spacing)
    slope = jnp.maximum(height - below, 0.0) / spacing
    ground = height - (surface_step * erodibility) * jnp.sqrt(drained) * slope
    base[...] = ground[RIM : RIM + NXL]

    finish_faces(ubuf, U_SET, 3)
    spread_rows(ubuf, U_SET, 3)
    for picard, count in enumerate(counts):
        def soften(x, held):
            for t in tiles_in:
                rate = rate_at(x, t)
                eta = jnp.minimum(visc[x, own(t)], strength[x, own(t)] / (2.0 * jnp.maximum(rate, rate_floor)))
                ebuf[0, x + 1, at(t), :] = eta
                held = pack(E_SET, 0, x, t, eta, held)
            return held

        keep_pack(E_SET, planes(soften, no_pack))
        start_faces(ebuf, E_SET, 1)
        finish_faces(ebuf, E_SET, 1)
        spread_rows(ebuf, E_SET, 1)
        lagged = count <= CUT + 1
        gram, rows_of = {}, ([], [])
        shift = {}

        def begin(x, carry):
            held, norm = carry
            for t in tiles_in:
                eta, pairs = around(ebuf, E_SET, 0, x, t)
                total = jnp.full((8, NZL), drag_coef, f32)
                ends = []
                for d in range(3):
                    for side in range(2):
                        face = 0.5 * (eta + pairs[d][side])
                        total = total + face
                        if d == 2:
                            ends.append(face)
                            face = jnp.where(lane_tile == (NZL - 1) * side, 0.0, face)
                        coef[2 * d + side, x, own(t)] = face
                coef[6, x, own(t)] = total
                coef[7, x, own(t)] = jnp.where(
                    lane_tile == edge, jnp.where(lane_tile == 0, ends[0], ends[1]), 0.0
                )
                for c in range(3):
                    _, au = applied(ubuf, U_SET, c, x, t)
                    tile = force[c, x, own(t)] - au
                    bbuf[0, c, x + 1, at(t), :] = tile
                    norm = norm + tile * tile
                    held = pack(0, c, x, t, tile, held)
            return held, norm

        held, norm = planes(begin, (no_pack, none), 1)
        keep_pack(0, held)
        keep_dots(0, rows_of[0], [(0, 0)], [norm])
        start_faces(bbuf.at[0], 0, 3)
        early = 2 * picard
        for k in range(count):
            if k != CUT:
                finish_faces(bbuf.at[k], k, 3)
                spread_rows(bbuf.at[k], k, 3)
            if lagged and k == CUT - 1:
                middle_sums(early)
            stored = k + 1 < count
            extra = {}
            if k >= CUT:
                extra[k] = alpha
                if k == CUT:
                    for m in range(CUT):
                        extra[m] = beta * turn[CUT - 1][m]
                else:
                    extra[k - 1] = beta
            partners = [m for m in range(k + 2 if stored else k + 1)]
            if k + 1 == CUT and lagged:
                partners = []

            def grow(x, carry):
                held, sums = carry
                sums = list(sums)
                for t in tiles_in:
                    for c in range(3):
                        v, w = applied(bbuf.at[k], k, c, x, t)
                        mine = {}
                        for m in sorted(set(extra) | set(partners)):
                            if m <= k:
                                mine[m] = v if m == k else bbuf[m, c, x + 1, at(t), :]
                        for m in sorted(extra):
                            w = w - extra[m] * mine[m]
                        mine[k + 1] = w
                        if stored:
                            bbuf[k + 1, c, x + 1, at(t), :] = w
                            held = pack(k + 1, c, x, t, w, held)
                        for spot, m in enumerate(partners):
                            sums[spot] = sums[spot] + mine[m] * w
                return held, tuple(sums)

            held, sums = planes(grow, (no_pack, tuple(none for _ in partners)))
            shift[k] = dict(extra)
            bank = 0 if k + 1 < CUT or (k + 1 == CUT and not lagged) else 1
            keep_dots(bank, rows_of[bank], [(m, k + 1) for m in partners], sums)
            if k + 1 == (CUT - 1 if lagged else CUT):
                start_sums(early, 0)
            if stored:
                keep_pack(k + 1, held)
                start_faces(bbuf.at[k + 1], k + 1, 3)
            if k + 1 == CUT:
                if not lagged:
                    middle_sums(early)
                finish_faces(bbuf.at[CUT], CUT, 3)
                finish_sums(early, rows_of[0], gram)
                turn, norms = lanczos(gram, CUT - 1 if lagged else CUT)
                top = CUT - 1 if lagged else CUT
                beta = norms[top] / norms[top - 1]
                alpha = turn[top - 1][top - 2] - turn[top][top - 1]
                if lagged:
                    full = [0.0] * (CUT + 1)
                    for m in range(CUT):
                        full[m + 1] = full[m + 1] + turn[top][m]
                        full[m] = full[m] - alpha * turn[top][m]
                    for m in range(CUT - 1):
                        full[m] = full[m] - beta * turn[top - 1][m]
                    mix = [-full[m] for m in range(CUT)]
                else:
                    mix = [-turn[CUT][m] for m in range(CUT)]
                shift[CUT - 1] = dict(enumerate(mix))
                straighten(mix, rows_of[1])
                spread_rows(bbuf.at[CUT], CUT, 3)

        start_sums(early + 1, 1)
        final = picard == len(counts) - 1
        if final:
            send_depth_sums(count)
        middle_sums(early + 1)
        finish_sums(early + 1, rows_of[1], gram)
        steps = solve(gram, shift, count)

        def total_of(first, parts):
            for step, part in zip(steps, parts):
                first = first + step * part
            return first

        for rim_of in (0, NXL + 1):
            for c in range(3):
                ubuf[c, rim_of, LO:HI, :] = total_of(
                    ubuf[c, rim_of, LO:HI, :], [bbuf[m, c, rim_of, LO:HI, :] for m in range(count)]
                )
        for side in range(2):
            for c in range(3):
                yr[U_SET, side, c] = total_of(yr[U_SET, side, c], [yr[m, side, c] for m in range(count)])
        zr[U_SET] = total_of(zr[U_SET], [zr[m] for m in range(count)])

        def settle(x, _):
            for c in range(3):
                for t in tiles_in:
                    tile = total_of(
                        ubuf[c, x + 1, at(t), :], [bbuf[m, c, x + 1, at(t), :] for m in range(count)]
                    )
                    ubuf[c, x + 1, at(t), :] = tile
                    if final:
                        vout[c, x, own(t)] = tile
            return 0

        planes(settle, 0)
        spread_rows(ubuf, U_SET, 3)

    def harden(x, _):
        for t in tiles_in:
            plastic = jnp.maximum(rate_at(x, t) - strength[x, own(t)] / (2.0 * visc[x, own(t)]), 0.0)
            sout[x, own(t)] = strain[x, own(t)] + strain_step * plastic
        return 0

    planes(harden, 0)
    tile_copy(slice(0, group - 1), 1).wait()
    scale = surface_step * uplift_gain / (pz * NZL)
    lane_group = lax.broadcasted_iota(jnp.int32, (1, NZL), 1) // NYL
    weights = []
    parts = [jnp.ones((1, NZL), f32)] + steps
    for t in range(2):
        weight = jnp.zeros((1, NZL), f32)
        for g, part in enumerate(parts[t * across : (t + 1) * across]):
            weight = jnp.where(lane_group == g, scale * part, weight)
        weights.append(weight)
    spread_group = lanes(NXL) // NYL
    for part in range(py // across):
        span = slice(part * NZL, (part + 1) * NZL)
        ground = base[:, span]
        for g in range(across):
            total = jnp.zeros((NXL, NZL), f32)
            for k in range(pz):
                for t in range(2):
                    total = total + weights[t] * tiles[(part * across + g) * pz + k, t]
            total = total + pltpu.roll(total, NZL // 2, 1)
            total = total + pltpu.roll(total, NYL, 1)
            ground = ground + jnp.where(spread_group == g, total, 0.0)
        tout[:, span] = ground


def build(counts, ident, px, py, pz, name):
    field = (3, NXL, NYL, NZL)
    cell = (NXL, NYL, NZL)
    cols = py * NYL
    group = py * pz
    dma = pltpu.SemaphoreType.DMA
    vmem = pl.BlockSpec(memory_space=pltpu.VMEM)
    return pl.pallas_call(
        functools.partial(step_kernel, counts, px, py, pz),
        out_shape=[
            jax.ShapeDtypeStruct(field, f32),
            jax.ShapeDtypeStruct(cell, f32),
            jax.ShapeDtypeStruct((NXL, cols), f32),
        ],
        in_specs=[pl.BlockSpec(memory_space=pl.ANY)] * 7,
        out_specs=[vmem] * 3,
        scratch_shapes=[
            pltpu.VMEM(field, f32),
            pltpu.VMEM(cell, f32),
            pltpu.VMEM(cell, f32),
            pltpu.VMEM(cell, jnp.int32),
            pltpu.VMEM((NXL, cols), f32),
            pltpu.VMEM((NXL, cols), jnp.int32),
            dma((7,)),
            pltpu.VMEM((3, NXL + 2, BUFY, NZL), f32),
            pltpu.VMEM((1, NXL + 2, BUFY, NZL), f32),
            pltpu.VMEM((KMAX, 3, NXL + 2, BUFY, NZL), f32),
            pltpu.VMEM((KMAX + 2, 2, 3, NXL, NZL), f32),
            pltpu.VMEM((KMAX + 2, 2, 3, NXL, NZL), f32),
            pltpu.VMEM((KMAX + 2, NYL // 2, NZL), f32),
            pltpu.VMEM((KMAX + 2, NYL // 2, NZL), f32),
            pltpu.VMEM(cell, f32),
            pltpu.VMEM((8, *cell), f32),
            pltpu.VMEM((2, ROWS, NZL), f32),
            pltpu.VMEM((4, px, 1, NZL), f32),
            pltpu.VMEM((4, group, 1, NZL), f32),
            pltpu.VMEM((2, NXL + 2 * RIM, cols), f32),
            pltpu.VMEM((NXL, cols), f32),
            pltpu.VMEM((group, 2, NXL, NZL), f32),
            dma((5,)), dma((2, 5)),
            dma((1,)), dma((2,)),
            dma((1,)), dma((2,)),
            dma((2,)), dma((2,)),
            dma((1,)), dma((1,)),
        ],
        compiler_params=pltpu.CompilerParams(
            collective_id=ident, has_side_effects=True, vmem_limit_bytes=40 * 1024 * 1024
        ),
        name=name,
    )


def local(px, py, pz, force, vel, visc, strain, flags, counts, heights, receivers):
    long_first = build((KMAX, KMAX - 2), 0, px, py, pz, "long_first")
    short_first = build((KMAX - 2, KMAX), 1, px, py, pz, "short_first")
    args = (force, vel, visc, strain, flags, heights, receivers)
    out = lax.cond(counts[0] == KMAX, lambda *a: tuple(long_first(*a)), lambda *a: tuple(short_first(*a)), *args)
    return tuple(out)


def solution(mesh):
    px, py, pz = mesh.shape["mx"], mesh.shape["my"], mesh.shape["mz"]
    vector, scalar, rows = P(None, "mx", "my", "mz"), P("mx", "my", "mz"), P("mx", None)
    return jax.shard_map(
        functools.partial(local, px, py, pz),
        mesh=mesh,
        in_specs=(vector, vector, scalar, scalar, scalar, P(), rows, rows),
        out_specs=(vector, scalar, rows),
        check_vma=False,
    )
```

```python
import functools
import math

import jax
import jax.numpy as jnp
from jax import lax
from jax.experimental import pallas as pl
from jax.experimental.pallas import tpu as pltpu
from jax.sharding import PartitionSpec as P

KMAX = 6
SWEEPS = 4
NXL, NYL, NZL = 16, 32, 128
PADY = 8
LO, HI = PADY, PADY + NYL
BUFY = PADY + NYL + PADY
RIM = 8

drag_coef = 0.05
cohesion_base = 1.0
weakening = 0.6
critical_strain = 1.0
sin_friction = 0.5
cos_friction = 0.8660254
pressure_gradient = 2.0
rate_floor = 0.1
strain_step = 0.5
uplift_gain = 8.0
surface_step = 0.2
erodibility = 0.5
neighbour_steps = ((-1, -1), (-1, 0), (-1, 1), (0, -1), (0, 1), (1, -1), (1, 0), (1, 1))

MESH = pl.DeviceIdType.MESH
U_SET, E_SET = KMAX, KMAX + 1
CUT = 3
ROWS = 32
f32 = jnp.float32


def lanczos(gram, top):
    turn, norms = [], []
    for i in range(top + 1):
        row = [0.0] * i + [1.0]
        for j in range(i):
            part = gram[i, j]
            for k in range(j):
                part = part + turn[j][k] * gram[i, k]
            part = part / norms[j]
            for k in range(j + 1):
                row[k] = row[k] - part * turn[j][k]
        norm = gram[i, i]
        for k in range(i):
            norm = norm + row[k] * gram[i, k]
        turn.append(row)
        norms.append(norm)
    return turn, norms


def solve(gram, shift, n):
    lower, pivots, right = {}, [], []

    def entry(i, j):
        total = gram[i, j + 1]
        for m, part in shift[j].items():
            total = total + part * gram[i, m]
        return total

    for i in range(n):
        for j in range(i):
            part = entry(i, j)
            for k in range(j):
                part = part - lower[i, k] * lower[j, k] * pivots[k]
            lower[i, j] = part / pivots[j]
        pivot = entry(i, i)
        for k in range(i):
            pivot = pivot - lower[i, k] * lower[i, k] * pivots[k]
        pivots.append(pivot)
        part = gram[i, 0]
        for k in range(i):
            part = part - lower[i, k] * right[k]
        right.append(part)
    steps = [part / pivot for part, pivot in zip(right, pivots)]
    for i in reversed(range(n)):
        for k in range(i + 1, n):
            steps[i] = steps[i] - lower[k, i] * steps[k]
    return steps


def step_kernel(
    counts, px, py, pz,
    force_in, vel_in, visc_in, strain_in, flags_in, heights_in, receivers_in,
    vout, sout, tout,
    force, visc, strain, flags, heights, receivers, load_sem,
    ubuf, ebuf, bbuf, ys, yr, zs, zr, strength, coef, dots, sums1, sums2, surf, base, tiles,
    face_send, face_recv, one_send, one_recv, two_send, two_recv, surf_send, surf_recv, tile_send, tile_recv,
):
    mx, my, mz = lax.axis_index("mx"), lax.axis_index("my"), lax.axis_index("mz")
    group = py * pz
    place = my * pz + mz
    edge = (NZL - 1) * (1 - mz)

    def at_group(k):
        other = lax.rem(place + k, group)
        return {"my": other // pz, "mz": lax.rem(other, pz)}

    def at_row(k):
        return {"mx": lax.rem(mx + k, px)}

    def lanes(rows):
        return lax.broadcasted_iota(jnp.int32, (rows, NZL), 1)

    def blank(buf, parts):
        zero = jnp.zeros((NYL, NZL), f32)
        row = jnp.zeros((1, NZL), f32)

        def clear(i, _):
            for c in range(parts):
                buf[c, i, LO - 1 : LO, :] = row
                buf[c, i, HI : HI + 1, :] = row
            return 0

        lax.fori_loop(0, NXL + 2, clear, 0)
        for c in range(parts):
            buf[c, 0, LO:HI, :] = zero
            buf[c, NXL + 1, LO:HI, :] = zero

    loads = [
        pltpu.make_async_copy(src, dst, load_sem.at[k])
        for k, (src, dst) in enumerate((
            (vel_in, ubuf.at[:, 1 : NXL + 1, LO:HI, :]), (heights_in, heights), (receivers_in, receivers),
            (strain_in, strain), (flags_in, flags), (visc_in, visc), (force_in, force),
        ))
    ]
    for copy in loads:
        copy.start()

    blank(ubuf, 3)
    blank(ebuf, 1)

    def blank_one(k, _):
        blank(bbuf.at[k], 3)
        return 0

    lax.fori_loop(0, KMAX, blank_one, 0)
    dots[...] = jnp.zeros(dots.shape, f32)

    def blank_rows(kind, _):
        for side in range(2):
            for c in range(3):
                yr[kind, side, c] = jnp.zeros((NXL, NZL), f32)
        return 0

    lax.fori_loop(0, KMAX + 2, blank_rows, 0)
    rows, cols = surf.shape[1:]
    surf[0, 0:RIM, :] = jnp.full((RIM, cols), -1.0, f32)
    surf[0, RIM + NXL :, :] = jnp.full((RIM, cols), -1.0, f32)
    surf[1, 0:RIM, :] = jnp.zeros((RIM, cols), f32)
    surf[1, RIM + NXL :, :] = jnp.zeros((RIM, cols), f32)

    barrier = pltpu.get_barrier_semaphore()
    for k in range(1, px):
        pl.semaphore_signal(barrier, inc=1, device_id=at_row(k), device_id_type=MESH)
    for k in range(1, group):
        pl.semaphore_signal(barrier, inc=1, device_id=at_group(k), device_id_type=MESH)

    turn_of = {"start": 0, "finish": 0}

    def face_copy(turn, d, src, dst, device):
        return pltpu.make_async_remote_copy(
            src_ref=src, dst_ref=dst, send_sem=face_send.at[d], recv_sem=face_recv.at[turn, d],
            device_id=device, device_id_type=MESH,
        )

    def face_copies(buf, kind, n):
        comps = slice(0, n)
        return (
            (mx < px - 1, mx > 0, 0, buf.at[comps, NXL, LO:HI, :], buf.at[comps, 0, LO:HI, :], {"mx": mx + 1}),
            (mx > 0, mx < px - 1, 1, buf.at[comps, 1, LO:HI, :], buf.at[comps, NXL + 1, LO:HI, :], {"mx": mx - 1}),
            (my < py - 1, my > 0, 2, ys.at[kind, 1, comps], yr.at[kind, 0, comps], {"my": my + 1}),
            (my > 0, my < py - 1, 3, ys.at[kind, 0, comps], yr.at[kind, 1, comps], {"my": my - 1}),
        )

    def depth_copy(turn, kind):
        return face_copy(turn, 4, zs.at[kind], zr.at[kind], {"mz": 1 - mz})

    def start_faces(buf, kind, n):
        turn = turn_of["start"] % 2
        turn_of["start"] += 1
        depth_copy(turn, kind).start()
        for sends, _, d, src, dst, device in face_copies(buf, kind, n):
            @pl.when(sends)
            def _():
                face_copy(turn, d, src, dst, device).start()

    def finish_faces(buf, kind, n):
        turn = turn_of["finish"] % 2
        turn_of["finish"] += 1
        for sends, receives, d, src, dst, device in face_copies(buf, kind, n):
            @pl.when(sends)
            def _():
                face_copy(turn, d, src, dst, device).wait_send()

            @pl.when(receives)
            def _():
                face_copy(turn, d, src, dst, device).wait_recv()
        depth_copy(turn, kind).wait()

    def spread_rows(buf, kind, n):
        def spread(x, _):
            for c in range(n):
                buf[c, x + 1, LO - 1 : LO, :] = yr[kind, 0, c, pl.ds(x, 1), :]
                buf[c, x + 1, HI : HI + 1, :] = yr[kind, 1, c, pl.ds(x, 1), :]
            return 0

        lax.fori_loop(0, NXL, spread, 0, unroll=4)

    lane_full = lanes(NYL)
    lane_tile = lanes(8)
    tiles_in = range(NYL // 8)

    def at(t, step=0):
        return slice(LO + 8 * t + step, LO + 8 * t + step + 8)

    def own(t):
        return slice(8 * t, 8 * t + 8)

    def pack(kind, c, x, t, tile, held):
        if t == 0:
            ys[kind, 0, c, pl.ds(x, 1), :] = tile[0:1]
        if t == NYL // 8 - 1:
            ys[kind, 1, c, pl.ds(x, 1), :] = tile[7:8]
        spot = c * NXL + x + 48 * (t // 2)
        turned = pltpu.roll(tile, spot - edge + NZL, 1)
        held = list(held)
        held[t % 2] = jnp.where(lane_tile == spot, turned, held[t % 2])
        return tuple(held)

    none = jnp.zeros((8, NZL), f32)
    no_pack = (none, none)

    def keep_pack(kind, held):
        zs[kind, 0:8] = held[0]
        zs[kind, 8:16] = held[1]

    def turned_rim(kind, c, x, t):
        spot = c * NXL + x + 48 * (t // 2)
        return pltpu.roll(zr[kind, own(t % 2)], edge - spot + NZL, 1)

    def around(buf, kind, c, x, t):
        v = buf[c, x + 1, at(t), :]
        rim = jnp.where(lane_tile == edge, turned_rim(kind, c, x, t), 0.0)
        below = jnp.where(lane_tile == 0, rim, pltpu.roll(v, 1, 1))
        above = jnp.where(lane_tile == NZL - 1, rim, pltpu.roll(v, NZL - 1, 1))
        return v, (
            (buf[c, x, at(t), :], buf[c, x + 2, at(t), :]),
            (buf[c, x + 1, at(t, -1), :], buf[c, x + 1, at(t, 1), :]),
            (below, above),
        )

    def applied(buf, kind, c, x, t):
        v = buf[c, x + 1, at(t), :]
        total = coef[6, x, own(t)] * v
        total = total - coef[0, x, own(t)] * buf[c, x, at(t), :] - coef[1, x, own(t)] * buf[c, x + 2, at(t), :]
        total = total - coef[2, x, own(t)] * buf[c, x + 1, at(t, -1), :]
        total = total - coef[3, x, own(t)] * buf[c, x + 1, at(t, 1), :]
        total = total - coef[4, x, own(t)] * pltpu.roll(v, 1, 1) - coef[5, x, own(t)] * pltpu.roll(v, NZL - 1, 1)
        return v, total - coef[7, x, own(t)] * turned_rim(kind, c, x, t)

    def rate_at(x, t):
        g = []
        for c in range(3):
            _, pairs = around(ubuf, U_SET, c, x, t)
            g.append([0.5 * (pair[1] - pair[0]) for pair in pairs])
        total = g[0][0] * g[0][0] + g[1][1] * g[1][1] + g[2][2] * g[2][2]
        for a, b in ((0, 1), (0, 2), (1, 2)):
            shear = g[a][b] + g[b][a]
            total = total + 0.5 * (shear * shear)
        return jnp.sqrt(0.5 * total)

    def planes(body, carry, unroll=4):
        return lax.fori_loop(0, NXL, body, carry, unroll=unroll)

    def sum_copy(sums, slot, mine, send, recv, device):
        ref = sums.at[slot, mine]
        return pltpu.make_async_remote_copy(
            src_ref=ref, dst_ref=ref, send_sem=send, recv_sem=recv, device_id=device, device_id_type=MESH
        )

    def one_copy(slot, mine, k):
        return sum_copy(sums1, slot, mine, one_send.at[0], one_recv.at[slot % 2], at_row(k))

    def two_copy(slot, mine, k):
        return sum_copy(sums2, slot, mine, two_send.at[0], two_recv.at[slot % 2], at_group(k))

    def start_sums(slot, bank):
        spot = lax.broadcasted_iota(jnp.int32, (ROWS, NZL), 0) == lanes(ROWS)
        line = jnp.sum(dots[bank], axis=1, keepdims=True)
        sums1[slot, mx] = jnp.sum(jnp.where(spot, line, 0.0), axis=0, keepdims=True)
        for k in range(1, px):
            one_copy(slot, mx, k).start()

    def middle_sums(slot):
        one_copy(slot, slice(0, px - 1), 1).wait()
        sums2[slot, place] = jnp.sum(sums1[slot], axis=0)
        for k in range(1, group):
            two_copy(slot, place, k).start()

    def finish_sums(slot, names, gram):
        two_copy(slot, slice(0, group - 1), 1).wait()
        total = jnp.sum(sums2[slot], axis=0)
        for spot, (i, j) in enumerate(names):
            gram[i, j] = gram[j, i] = jnp.broadcast_to(total[:, spot : spot + 1], (1, NZL))

    def keep_dots(bank, names, pairs, sums):
        for pair, total in zip(pairs, sums):
            spot = len(names)
            dots[bank, spot : spot + 1, :] = jnp.sum(total, axis=0, keepdims=True)
            names.append(pair)

    def straighten(mix, names):
        pairs = [(m, CUT) for m in range(CUT + 1)]
        for rim_of in (0, NXL + 1):
            for c in range(3):
                plane = bbuf[CUT, c, rim_of, LO:HI, :]
                for m in range(CUT):
                    plane = plane - mix[m] * bbuf[m, c, rim_of, LO:HI, :]
                bbuf[CUT, c, rim_of, LO:HI, :] = plane
        for side in range(2):
            for c in range(3):
                face = yr[CUT, side, c]
                for m in range(CUT):
                    face = face - mix[m] * yr[m, side, c]
                yr[CUT, side, c] = face
        face = zr[CUT]
        for m in range(CUT):
            face = face - mix[m] * zr[m]
        zr[CUT] = face

        def one(x, sums):
            sums = list(sums)
            for t in tiles_in:
                for c in range(3):
                    mine = [bbuf[m, c, x + 1, at(t), :] for m in range(CUT)]
                    tile = bbuf[CUT, c, x + 1, at(t), :]
                    for m in range(CUT):
                        tile = tile - mix[m] * mine[m]
                    bbuf[CUT, c, x + 1, at(t), :] = tile
                    mine.append(tile)
                    for m in range(CUT + 1):
                        sums[m] = sums[m] + mine[m] * tile
            return tuple(sums)

        sums = planes(one, (none,) * (CUT + 1))
        keep_dots(1, names, pairs, sums)

    across = NZL // NYL

    def tile_copy(mine, k):
        ref = tiles.at[mine]
        return pltpu.make_async_remote_copy(
            src_ref=ref, dst_ref=ref, send_sem=tile_send.at[0], recv_sem=tile_recv.at[0],
            device_id=at_group(k), device_id_type=MESH,
        )

    def send_depth_sums(count):
        tall = jnp.zeros((NYL, NZL), f32)

        def add_up(x, sums):
            fields = [ubuf[2, x + 1, LO:HI, :]] + [bbuf[m, 2, x + 1, LO:HI, :] for m in range(count)]
            return tuple(
                jnp.where(lane_full == x, jnp.sum(plane, axis=1, keepdims=True), old)
                for plane, old in zip(fields, sums)
            )

        sums = list(planes(add_up, (tall,) * (count + 1), 1)) + [tall] * (2 * across - count - 1)
        for t in range(2):
            square = jnp.concatenate(sums[t * across : (t + 1) * across], axis=0)
            tiles[place, t] = jnp.transpose(square)[0:NXL]

    def start_tiles():
        for k in range(1, group):
            tile_copy(place, k).start()

    def load(x, held):
        for c in range(3):
            for t in tiles_in:
                held = pack(U_SET, c, x, t, ubuf[c, x + 1, at(t), :], held)
        return held

    loads[0].wait()
    keep_pack(U_SET, planes(load, no_pack))
    pl.semaphore_wait(barrier, px - 1 + group - 1)
    start_faces(ubuf, U_SET, 3)

    def surf_copy(d):
        if d == 0:
            src, dst, device = surf.at[:, NXL : NXL + RIM], surf.at[:, 0:RIM], {"mx": mx + 1}
        else:
            src, dst, device = surf.at[:, RIM : 2 * RIM], surf.at[:, RIM + NXL : RIM + NXL + RIM], {"mx": mx - 1}
        return pltpu.make_async_remote_copy(
            src_ref=src, dst_ref=dst, send_sem=surf_send.at[d], recv_sem=surf_recv.at[d],
            device_id=device, device_id_type=MESH,
        )

    for copy in loads[1:]:
        copy.wait()
    surf[0, RIM : RIM + NXL, :] = receivers[...].astype(f32)
    surf[1, RIM : RIM + NXL, :] = heights[...]
    for d, sends in ((0, mx < px - 1), (1, mx > 0)):
        @pl.when(sends)
        def _():
            surf_copy(d).start()

    depth_at = mz * NZL + lane_full
    pressure = pressure_gradient * (pz * NZL - 0.5 - depth_at.astype(f32)) / (pz * NZL)

    def strengthen(x, _):
        weak = flags[x].astype(f32) * jnp.minimum(strain[x] / critical_strain, 1.0)
        strength[x] = cohesion_base * (1.0 - weakening * weak) * cos_friction + pressure * sin_friction
        return 0

    planes(strengthen, 0)

    for d, sends, receives in ((0, mx < px - 1, mx > 0), (1, mx > 0, mx < px - 1)):
        @pl.when(sends)
        def _():
            surf_copy(d).wait_send()

        @pl.when(receives)
        def _():
            surf_copy(d).wait_recv()

    code = surf[0]
    col = lax.broadcasted_iota(jnp.int32, (rows, cols), 1)

    def turned(block, row_step, col_step):
        if col_step:
            block = pltpu.roll(block, col_step % cols, 1)
        if row_step:
            block = pltpu.roll(block, row_step % rows, 0)
        return block

    def sweep(_, drained):
        total = jnp.ones((rows, cols), f32)
        for direction, (row_step, col_step) in enumerate(neighbour_steps):
            chosen = code == float(direction)
            if col_step:
                chosen = chosen & (col != (cols - 1 if col_step > 0 else 0))
            total = total + turned(jnp.where(chosen, drained, 0.0), row_step, col_step)
        return total

    drained = lax.fori_loop(0, SWEEPS, sweep, jnp.ones((rows, cols), f32))
    height = surf[1]
    below = jnp.zeros((rows, cols), f32)
    spacing = jnp.ones((rows, cols), f32)
    for direction, (row_step, col_step) in enumerate(neighbour_steps):
        chosen = code == float(direction)
        seen = chosen
        if col_step:
            seen = seen & (col != (cols - 1 if col_step > 0 else 0))
        below = below + jnp.where(seen, turned(height, -row_step, -col_step), 0.0)
        if row_step and col_step:
            spacing = jnp.where(chosen, math.sqrt(2.0), spacing)
    slope = jnp.maximum(height - below, 0.0) / spacing
    ground = height - (surface_step * erodibility) * jnp.sqrt(drained) * slope
    base[...] = ground[RIM : RIM + NXL]

    finish_faces(ubuf, U_SET, 3)
    spread_rows(ubuf, U_SET, 3)
    for picard, count in enumerate(counts):
        def soften(x, held):
            for t in tiles_in:
                rate = rate_at(x, t)
                eta = jnp.minimum(visc[x, own(t)], strength[x, own(t)] / (2.0 * jnp.maximum(rate, rate_floor)))
                ebuf[0, x + 1, at(t), :] = eta
                held = pack(E_SET, 0, x, t, eta, held)
            return held

        keep_pack(E_SET, planes(soften, no_pack))
        start_faces(ebuf, E_SET, 1)
        finish_faces(ebuf, E_SET, 1)
        spread_rows(ebuf, E_SET, 1)
        lagged = count <= CUT + 1
        gram, rows_of = {}, ([], [])
        shift = {}

        def begin(x, carry):
            held, norm = carry
            for t in tiles_in:
                eta, pairs = around(ebuf, E_SET, 0, x, t)
                total = jnp.full((8, NZL), drag_coef, f32)
                ends = []
                for d in range(3):
                    for side in range(2):
                        face = 0.5 * (eta + pairs[d][side])
                        total = total + face
                        if d == 2:
                            ends.append(face)
                            face = jnp.where(lane_tile == (NZL - 1) * side, 0.0, face)
                        coef[2 * d + side, x, own(t)] = face
                coef[6, x, own(t)] = total
                coef[7, x, own(t)] = jnp.where(
                    lane_tile == edge, jnp.where(lane_tile == 0, ends[0], ends[1]), 0.0
                )
                for c in range(3):
                    _, au = applied(ubuf, U_SET, c, x, t)
                    tile = force[c, x, own(t)] - au
                    bbuf[0, c, x + 1, at(t), :] = tile
                    norm = norm + tile * tile
                    held = pack(0, c, x, t, tile, held)
            return held, norm

        held, norm = planes(begin, (no_pack, none), 1)
        keep_pack(0, held)
        keep_dots(0, rows_of[0], [(0, 0)], [norm])
        start_faces(bbuf.at[0], 0, 3)
        early = 2 * picard
        for k in range(count):
            if k != CUT:
                finish_faces(bbuf.at[k], k, 3)
                spread_rows(bbuf.at[k], k, 3)
            if lagged and k == CUT - 1:
                middle_sums(early)
            stored = k + 1 < count
            extra = {}
            if k >= CUT:
                extra[k] = alpha
                if k == CUT:
                    for m in range(CUT):
                        extra[m] = beta * turn[CUT - 1][m]
                else:
                    extra[k - 1] = beta
            partners = [m for m in range(k + 2 if stored else k + 1)]
            if k + 1 == CUT and lagged:
                partners = []

            def grow(x, carry):
                held, sums = carry
                sums = list(sums)
                for t in tiles_in:
                    for c in range(3):
                        v, w = applied(bbuf.at[k], k, c, x, t)
                        mine = {}
                        for m in sorted(set(extra) | set(partners)):
                            if m <= k:
                                mine[m] = v if m == k else bbuf[m, c, x + 1, at(t), :]
                        for m in sorted(extra):
                            w = w - extra[m] * mine[m]
                        mine[k + 1] = w
                        if stored:
                            bbuf[k + 1, c, x + 1, at(t), :] = w
                        for spot, m in enumerate(partners):
                            sums[spot] = sums[spot] + mine[m] * w
                return held, tuple(sums)

            held, sums = planes(grow, (no_pack, tuple(none for _ in partners)))
            if stored:
                def wrap(x, held):
                    for c in range(3):
                        for t in tiles_in:
                            held = pack(k + 1, c, x, t, bbuf[k + 1, c, x + 1, at(t), :], held)
                    return held

                held = planes(wrap, held, 4)
            shift[k] = dict(extra)
            bank = 0 if k + 1 < CUT or (k + 1 == CUT and not lagged) else 1
            keep_dots(bank, rows_of[bank], [(m, k + 1) for m in partners], sums)
            if k + 1 == (CUT - 1 if lagged else CUT):
                start_sums(early, 0)
            if stored:
                keep_pack(k + 1, held)
                start_faces(bbuf.at[k + 1], k + 1, 3)
            if k + 1 == CUT:
                if not lagged:
                    middle_sums(early)
                finish_faces(bbuf.at[CUT], CUT, 3)
                finish_sums(early, rows_of[0], gram)
                turn, norms = lanczos(gram, CUT - 1 if lagged else CUT)
                top = CUT - 1 if lagged else CUT
                beta = norms[top] / norms[top - 1]
                alpha = turn[top - 1][top - 2] - turn[top][top - 1]
                if lagged:
                    full = [0.0] * (CUT + 1)
                    for m in range(CUT):
                        full[m + 1] = full[m + 1] + turn[top][m]
                        full[m] = full[m] - alpha * turn[top][m]
                    for m in range(CUT - 1):
                        full[m] = full[m] - beta * turn[top - 1][m]
                    mix = [-full[m] for m in range(CUT)]
                else:
                    mix = [-turn[CUT][m] for m in range(CUT)]
                shift[CUT - 1] = dict(enumerate(mix))
                straighten(mix, rows_of[1])
                spread_rows(bbuf.at[CUT], CUT, 3)

        start_sums(early + 1, 1)
        final = picard == len(counts) - 1
        if final:
            send_depth_sums(count)
        middle_sums(early + 1)
        if final:
            start_tiles()
        finish_sums(early + 1, rows_of[1], gram)
        steps = solve(gram, shift, count)

        def total_of(first, parts):
            for step, part in zip(steps, parts):
                first = first + step * part
            return first

        for rim_of in (0, NXL + 1):
            for c in range(3):
                ubuf[c, rim_of, LO:HI, :] = total_of(
                    ubuf[c, rim_of, LO:HI, :], [bbuf[m, c, rim_of, LO:HI, :] for m in range(count)]
                )
        for side in range(2):
            for c in range(3):
                yr[U_SET, side, c] = total_of(yr[U_SET, side, c], [yr[m, side, c] for m in range(count)])
        zr[U_SET] = total_of(zr[U_SET], [zr[m] for m in range(count)])

        def settle(x, _):
            for c in range(3):
                for t in tiles_in:
                    tile = total_of(
                        ubuf[c, x + 1, at(t), :], [bbuf[m, c, x + 1, at(t), :] for m in range(count)]
                    )
                    ubuf[c, x + 1, at(t), :] = tile
                    if final:
                        vout[c, x, own(t)] = tile
            return 0

        planes(settle, 0)
        spread_rows(ubuf, U_SET, 3)

    def harden(x, _):
        for t in tiles_in:
            plastic = jnp.maximum(rate_at(x, t) - strength[x, own(t)] / (2.0 * visc[x, own(t)]), 0.0)
            sout[x, own(t)] = strain[x, own(t)] + strain_step * plastic
        return 0

    planes(harden, 0)
    tile_copy(slice(0, group - 1), 1).wait()
    scale = surface_step * uplift_gain / (pz * NZL)
    lane_group = lax.broadcasted_iota(jnp.int32, (1, NZL), 1) // NYL
    weights = []
    parts = [jnp.ones((1, NZL), f32)] + steps
    for t in range(2):
        weight = jnp.zeros((1, NZL), f32)
        for g, part in enumerate(parts[t * across : (t + 1) * across]):
            weight = jnp.where(lane_group == g, scale * part, weight)
        weights.append(weight)
    spread_group = lanes(NXL) // NYL
    for part in range(py // across):
        span = slice(part * NZL, (part + 1) * NZL)
        ground = base[:, span]
        for g in range(across):
            total = jnp.zeros((NXL, NZL), f32)
            for k in range(pz):
                for t in range(2):
                    total = total + weights[t] * tiles[(part * across + g) * pz + k, t]
            total = total + pltpu.roll(total, NZL // 2, 1)
            total = total + pltpu.roll(total, NYL, 1)
            ground = ground + jnp.where(spread_group == g, total, 0.0)
        tout[:, span] = ground


def build(counts, ident, px, py, pz, name):
    field = (3, NXL, NYL, NZL)
    cell = (NXL, NYL, NZL)
    cols = py * NYL
    group = py * pz
    dma = pltpu.SemaphoreType.DMA
    vmem = pl.BlockSpec(memory_space=pltpu.VMEM)
    return pl.pallas_call(
        functools.partial(step_kernel, counts, px, py, pz),
        out_shape=[
            jax.ShapeDtypeStruct(field, f32),
            jax.ShapeDtypeStruct(cell, f32),
            jax.ShapeDtypeStruct((NXL, cols), f32),
        ],
        in_specs=[pl.BlockSpec(memory_space=pl.ANY)] * 7,
        out_specs=[vmem] * 3,
        scratch_shapes=[
            pltpu.VMEM(field, f32),
            pltpu.VMEM(cell, f32),
            pltpu.VMEM(cell, f32),
            pltpu.VMEM(cell, jnp.int32),
            pltpu.VMEM((NXL, cols), f32),
            pltpu.VMEM((NXL, cols), jnp.int32),
            dma((7,)),
            pltpu.VMEM((3, NXL + 2, BUFY, NZL), f32),
            pltpu.VMEM((1, NXL + 2, BUFY, NZL), f32),
            pltpu.VMEM((KMAX, 3, NXL + 2, BUFY, NZL), f32),
            pltpu.VMEM((KMAX + 2, 2, 3, NXL, NZL), f32),
            pltpu.VMEM((KMAX + 2, 2, 3, NXL, NZL), f32),
            pltpu.VMEM((KMAX + 2, NYL // 2, NZL), f32),
            pltpu.VMEM((KMAX + 2, NYL // 2, NZL), f32),
            pltpu.VMEM(cell, f32),
            pltpu.VMEM((8, *cell), f32),
            pltpu.VMEM((2, ROWS, NZL), f32),
            pltpu.VMEM((4, px, 1, NZL), f32),
            pltpu.VMEM((4, group, 1, NZL), f32),
            pltpu.VMEM((2, NXL + 2 * RIM, cols), f32),
            pltpu.VMEM((NXL, cols), f32),
            pltpu.VMEM((group, 2, NXL, NZL), f32),
            dma((5,)), dma((2, 5)),
            dma((1,)), dma((2,)),
            dma((1,)), dma((2,)),
            dma((2,)), dma((2,)),
            dma((1,)), dma((1,)),
        ],
        compiler_params=pltpu.CompilerParams(
            collective_id=ident, has_side_effects=True, vmem_limit_bytes=40 * 1024 * 1024
        ),
        name=name,
    )


def local(px, py, pz, force, vel, visc, strain, flags, counts, heights, receivers):
    long_first = build((KMAX, KMAX - 2), 0, px, py, pz, "long_first")
    short_first = build((KMAX - 2, KMAX), 1, px, py, pz, "short_first")
    args = (force, vel, visc, strain, flags, heights, receivers)
    out = lax.cond(counts[0] == KMAX, lambda *a: tuple(long_first(*a)), lambda *a: tuple(short_first(*a)), *args)
    return tuple(out)


def solution(mesh):
    px, py, pz = mesh.shape["mx"], mesh.shape["my"], mesh.shape["mz"]
    vector, scalar, rows = P(None, "mx", "my", "mz"), P("mx", "my", "mz"), P("mx", None)
    return jax.shard_map(
        functools.partial(local, px, py, pz),
        mesh=mesh,
        in_specs=(vector, vector, scalar, scalar, scalar, P(), rows, rows),
        out_specs=(vector, scalar, rows),
        check_vma=False,
    )
```
